32 devices in a mesh: member: 1 (over z), ty: 4 (over y), tx: 4 (over x), panel: 2 (over core).
Axes of the slice: x: 4, y: 4, z: 1, core: 2. Of those that a mesh axis runs over, the one named last changes fastest.
The devices are a block of a 4x4x8 slice.
Arguments:
- height: float32 [6, 768, 768], P(('member', 'panel'), 'tx', 'ty')
- wind_u: float32 [6, 768, 768], P(('member', 'panel'), 'tx', 'ty')
- wind_v: float32 [6, 768, 768], P(('member', 'panel'), 'tx', 'ty')
- sqrt_g: float32 [6, 768, 768], P('panel', 'tx', 'ty')
- metric_aa: float32 [6, 768, 768], P('panel', 'tx', 'ty')
- metric_ab: float32 [6, 768, 768], P('panel', 'tx', 'ty')
- metric_bb: float32 [6, 768, 768], P('panel', 'tx', 'ty')
- coriolis: float32 [6, 768, 768], P('panel', 'tx', 'ty')
- topography: float32 [6, 768, 768], P('panel', 'tx', 'ty')
- rotation: float32 [6, 4, 768, 2, 2], P('panel')
- tracers: float32 [8, 6, 768, 768], P(None, ('member', 'panel'), 'tx', 'ty')
Outputs:
- output 1: float32 [6, 768, 768], P(('member', 'panel'), 'tx', 'ty')
- output 2: float32 [6, 768, 768], P(('member', 'panel'), 'tx', 'ty')
- output 3: float32 [6, 768, 768], P(('member', 'panel'), 'tx', 'ty')
- output 4: float32 [8, 6, 768, 768], P(None, ('member', 'panel'), 'tx', 'ty')
All inputs are finite; a program needn't handle non-finite values.
Results may differ from the reference program's by a relative error of at most 0.001.
Values sent between devices are 32-bit elements.
A program may use at most 768 MiB of HBM per device.

```python
import jax
import jax.numpy as jnp
from jax import lax

N = 768
TRACERS = 8
STEPS = 8

TIME_STEP = 0.1
GRAVITY = 1.0
WAVE_SPEED = 1.0
TWO_PI = 6.283185307179586
NEIGHBOURS = (
    ((3, 1, 0), (1, 0, 0), (5, 3, 0), (4, 2, 0)),
    ((0, 1, 0), (2, 0, 0), (5, 1, 1), (4, 1, 0)),
    ((1, 1, 0), (3, 0, 0), (5, 2, 1), (4, 3, 1)),
    ((2, 1, 0), (0, 0, 0), (5, 0, 0), (4, 0, 1)),
    ((3, 3, 1), (1, 3, 0), (0, 3, 0), (2, 3, 1)),
    ((3, 2, 0), (1, 2, 1), (2, 2, 1), (0, 2, 0)),
)


def edge_strips(tile_block):
    west_side = tile_block[..., 0:2, :]
    east_side = jnp.flip(tile_block[..., -2:, :], axis=-2)
    south_side = jnp.swapaxes(tile_block[..., :, 0:2], -1, -2)
    north_side = jnp.swapaxes(jnp.flip(tile_block[..., :, -2:], axis=-1), -1, -2)
    return jnp.stack([west_side, east_side, south_side, north_side], axis=-4)


def cross_ghosts(strip_set):
    panel_rows = []
    for panel_id in range(6):
        edge_list = []
        for edge_id in range(4):
            other_panel, other_edge, flipped = NEIGHBOURS[panel_id][edge_id]
            segment = strip_set[other_panel, other_edge]
            if flipped == 1:
                segment = jnp.flip(segment, axis=-1)
            edge_list.append(segment)
        panel_rows.append(jnp.stack(edge_list))
    return jnp.stack(panel_rows)


def rotate_wind(ghosts, rotation_part):
    wind_a = ghosts[..., 1, :, :]
    wind_b = ghosts[..., 2, :, :]
    matrix_part = rotation_part[..., None, :, :, :]
    new_a = matrix_part[..., 0, 0] * wind_a + matrix_part[..., 0, 1] * wind_b
    new_b = matrix_part[..., 1, 0] * wind_a + matrix_part[..., 1, 1] * wind_b
    return jnp.concatenate([ghosts[..., 0:1, :, :], new_a[..., None, :, :], new_b[..., None, :, :], ghosts[..., 3:, :, :]], axis=-3)


def mirror_ends(strip_part):
    return jnp.concatenate([jnp.flip(strip_part[..., 0:2], axis=-1), strip_part, jnp.flip(strip_part[..., -2:], axis=-1)], axis=-1)


def assemble(tile_block, ghosts):
    west_side = mirror_ends(jnp.flip(ghosts[..., 0, :, :, :], axis=-2))
    east_side = mirror_ends(ghosts[..., 1, :, :, :])
    south_side = jnp.swapaxes(jnp.flip(ghosts[..., 2, :, :, :], axis=-2), -1, -2)
    north_side = jnp.swapaxes(ghosts[..., 3, :, :, :], -1, -2)
    middle = jnp.concatenate([south_side, tile_block, north_side], axis=-1)
    return jnp.concatenate([west_side, middle, east_side], axis=-2)


def panel_halo(state, rotation):
    ghosts = cross_ghosts(edge_strips(state))
    if rotation is not None:
        ghosts = rotate_wind(ghosts, rotation)
    return assemble(state, ghosts)


def window(field_arr, shift_a, shift_b):
    row_count = field_arr.shape[-2] - 4
    col_count = field_arr.shape[-1] - 4
    return field_arr[..., 2 + shift_a:2 + shift_a + row_count, 2 + shift_b:2 + shift_b + col_count]


def tendency(ext_state, ext_static, coriolis):
    row_count = ext_state.shape[-2] - 4
    col_count = ext_state.shape[-1] - 4
    height = ext_state[:, 0]
    wind_a = ext_state[:, 1]
    wind_b = ext_state[:, 2]
    tracer = ext_state[:, 3:]
    jacobian = ext_static[:, 0]
    contra_a = ext_static[:, 1] * wind_a + ext_static[:, 2] * wind_b
    contra_b = ext_static[:, 2] * wind_a + ext_static[:, 3] * wind_b
    mass_a = jacobian * height * contra_a
    mass_b = jacobian * height * contra_b

    def faces_a(field_arr):
        return field_arr[..., 1:row_count + 2, 2:col_count + 2], field_arr[..., 2:row_count + 3, 2:col_count + 2]

    def faces_b(field_arr):
        return field_arr[..., 2:row_count + 2, 1:col_count + 2], field_arr[..., 2:row_count + 2, 2:col_count + 3]

    def diff_a(field_arr):
        return (window(field_arr, -2, 0) - 8.0 * window(field_arr, -1, 0) + 8.0 * window(field_arr, 1, 0) - window(field_arr, 2, 0)) / 12.0

    def diff_b(field_arr):
        return (window(field_arr, 0, -2) - 8.0 * window(field_arr, 0, -1) + 8.0 * window(field_arr, 0, 1) - window(field_arr, 0, 2)) / 12.0

    def lap_nine(field_arr):
        side_sum = window(field_arr, 1, 0) + window(field_arr, -1, 0) + window(field_arr, 0, 1) + window(field_arr, 0, -1)
        corner_sum = window(field_arr, 1, 1) + window(field_arr, 1, -1) + window(field_arr, -1, 1) + window(field_arr, -1, -1)
        return (4.0 * side_sum + corner_sum - 20.0 * window(field_arr, 0, 0)) / 6.0

    height_l, height_r = faces_a(height)
    mass_l, mass_r = faces_a(mass_a)
    flux_a = 0.5 * (mass_l + mass_r) - (0.5 * WAVE_SPEED) * (height_r - height_l)
    height_l, height_r = faces_b(height)
    mass_l, mass_r = faces_b(mass_b)
    flux_b = 0.5 * (mass_l + mass_r) - (0.5 * WAVE_SPEED) * (height_r - height_l)
    jac_centre = window(jacobian, 0, 0)
    inv_jac = 1.0 / jac_centre
    height_t = -((flux_a[..., 1:, :] - flux_a[..., :-1, :]) + (flux_b[..., 1:] - flux_b[..., :-1])) * inv_jac
    tracer_l, tracer_r = faces_a(tracer)
    tflux_a = flux_a[:, None] * (0.5 * (tracer_l + tracer_r)) - (0.5 * WAVE_SPEED) * (tracer_r - tracer_l)
    tracer_l, tracer_r = faces_b(tracer)
    tflux_b = flux_b[:, None] * (0.5 * (tracer_l + tracer_r)) - (0.5 * WAVE_SPEED) * (tracer_r - tracer_l)
    tracer_t = -((tflux_a[..., 1:, :] - tflux_a[..., :-1, :]) + (tflux_b[..., 1:] - tflux_b[..., :-1])) * inv_jac[:, None]
    energy = GRAVITY * (height + ext_static[:, 4]) + 0.5 * (wind_a * contra_a + wind_b * contra_b)
    vorticity = (diff_a(wind_b) - diff_b(wind_a)) * inv_jac + coriolis
    wind_a_t = -diff_a(energy) + vorticity * jac_centre * window(contra_b, 0, 0) + WAVE_SPEED * lap_nine(wind_a)
    wind_b_t = -diff_b(energy) - vorticity * jac_centre * window(contra_a, 0, 0) + WAVE_SPEED * lap_nine(wind_b)
    return jnp.concatenate([height_t[:, None], wind_a_t[:, None], wind_b_t[:, None], tracer_t], axis=1)


def expand_last(values):
    return values[..., None, None]


def wavy_field(base_key, lead):
    subkeys = jax.random.split(base_key, 3)
    centres = (jnp.arange(N, dtype=jnp.float32) + 0.5) / N
    coord_a = centres[:, None]
    coord_b = centres[None, :]
    amplitudes = jax.random.normal(subkeys[0], lead + (3,), jnp.float32)
    phases = jax.random.uniform(subkeys[1], lead + (3,), jnp.float32) * TWO_PI
    smooth = (expand_last(amplitudes[..., 0]) * jnp.sin(TWO_PI * (coord_a + coord_b) + expand_last(phases[..., 0]))
              + expand_last(amplitudes[..., 1]) * jnp.sin(TWO_PI * (2.0 * coord_a - coord_b) + expand_last(phases[..., 1]))
              + expand_last(amplitudes[..., 2]) * jnp.cos(TWO_PI * (coord_a + 3.0 * coord_b) + expand_last(phases[..., 2])))
    rough = jax.random.normal(subkeys[2], lead + (N, N), jnp.float32)
    return smooth, rough


def setup_inputs(seed: int = 0, part: int = 0) -> dict:
    base_key = jax.random.key(seed)
    shared = jax.random.split(base_key, 8)
    member_keys = jax.random.split(jax.random.fold_in(base_key, part), 4)
    box = (6, N, N)
    smooth, rough = wavy_field(member_keys[0], (6,))
    height = 1.0 + 0.1 * smooth + 0.05 * rough
    smooth, rough = wavy_field(member_keys[1], (6,))
    wind_u = 0.4 * smooth + 0.15 * rough
    smooth, rough = wavy_field(member_keys[2], (6,))
    wind_v = 0.4 * smooth + 0.15 * rough
    smooth, rough = wavy_field(member_keys[3], (TRACERS, 6))
    tracers = smooth + 0.3 * rough
    sqrt_g = 1.0 + 0.2 * jax.random.uniform(shared[0], box, jnp.float32, -1.0, 1.0)
    metric_aa = 1.0 + 0.2 * jax.random.uniform(shared[1], box, jnp.float32, -1.0, 1.0)
    metric_ab = 0.2 * jax.random.uniform(shared[2], box, jnp.float32, -1.0, 1.0)
    metric_bb = 1.0 + 0.2 * jax.random.uniform(shared[3], box, jnp.float32, -1.0, 1.0)
    smooth, rough = wavy_field(shared[4], (6,))
    coriolis = 0.6 * smooth + 0.2 * rough
    smooth, rough = wavy_field(shared[5], (6,))
    topography = 0.3 * smooth + 0.2 * rough
    angle = jax.random.uniform(shared[6], (6, 4, 1), jnp.float32, -1.2, 1.2) + 0.3 * jax.random.normal(shared[7], (6, 4, N), jnp.float32)
    cosine = jnp.cos(angle)
    sine = jnp.sin(angle)
    rotation = jnp.stack([jnp.stack([cosine, -sine], axis=-1), jnp.stack([sine, cosine], axis=-1)], axis=-2)
    return {'height': height, 'wind_u': wind_u, 'wind_v': wind_v, 'sqrt_g': sqrt_g, 'metric_aa': metric_aa, 'metric_ab': metric_ab, 'metric_bb': metric_bb, 'coriolis': coriolis, 'topography': topography, 'rotation': rotation, 'tracers': tracers}


def reference(height, wind_u, wind_v, sqrt_g, metric_aa, metric_ab, metric_bb, coriolis, topography, rotation, tracers):
    statics = jnp.stack([sqrt_g, metric_aa, metric_ab, metric_bb, topography], axis=1)
    ext_static = panel_halo(statics, None)
    state = jnp.concatenate([height[:, None], wind_u[:, None], wind_v[:, None], jnp.swapaxes(tracers, 0, 1)], axis=1)

    def rhs_of(current):
        return tendency(panel_halo(current, rotation), ext_static, coriolis)

    def one_step(step_index, current):
        first = current + TIME_STEP * rhs_of(current)
        return 0.5 * (current + first + TIME_STEP * rhs_of(first))

    final = lax.fori_loop(0, STEPS, one_step, state)
    return final[:, 0], final[:, 1], final[:, 2], jnp.swapaxes(final[:, 3:], 0, 1)
```

```python
import functools

import jax
import jax.numpy as jnp
from jax import lax
from jax.experimental import pallas as pl
from jax.experimental.pallas import tpu as pltpu
from jax.sharding import PartitionSpec as P

STEPS = 8
TIME_STEP = 0.1
GRAVITY = 1.0
WAVE_SPEED = 1.0
LINKS = (
    '310 100 530 420',
    '010 200 511 410',
    '110 300 521 431',
    '210 000 500 401',
    '331 130 030 231',
    '320 121 221 020',
)
NEIGHBOURS = tuple(tuple(tuple(map(int, link)) for link in row.split()) for row in LINKS)
LANES = 128
HALF = 96
TOP = 8
EDGES = 4
BASE = 3
DEPTH = 2
ROWS1 = 16
ROWS2 = 16
ROWSB = 32
ROWSP = 32
F32 = jnp.float32


def pick(index, values):
    if all(value is values[0] for value in values):
        return values[0]
    total = 0
    for place, value in enumerate(values):
        total = total + same(index, place) * value
    return total


def same(x, y):
    return 1 - lax.min((x - y) * (x - y), 1)


def mix(cond, yes, no):
    return cond * yes + (1 - cond) * no


def on_edge(edge, along, count):
    if edge == 0:
        return 0, along
    if edge == 1:
        return count - 1, along
    if edge == 2:
        return along, 0
    return along, count - 1


class Plan:
    def __init__(self, core, pos_a, pos_b, cores, count):
        self.core, self.pos_a, self.pos_b = core, pos_a, pos_b
        self.cores, self.count = cores, count
        self.slots = 6 // cores
        first = lambda x: 1 - lax.div(x + count - 1, count)
        last = lambda x: lax.div(x + 1, count)
        self.at_edge = (first(pos_a), last(pos_a), first(pos_b), last(pos_b))

    def across(self, slot, edge, along, side=None):
        found = []
        for core in range(self.cores):
            other, other_edge, flipped = NEIGHBOURS[core * self.slots + slot][edge]
            place = self.count - 1 - along if flipped else along
            tile_a, tile_b = on_edge(other_edge, place, self.count)
            if side is None:
                index = (other % self.slots) * EDGES + other_edge
            else:
                end = 1 - side if flipped else side
                if other_edge < 2:
                    index = (other % self.slots) * EDGES + 2 * other_edge + end
                else:
                    index = (other % self.slots) * EDGES + 2 * end + other_edge - 2
            found.append((other // self.slots, tile_a, tile_b, index))
        return tuple(pick(self.core, [entry[k] for entry in found]) for k in range(EDGES))

    def edge(self, slot, edge):
        along = self.pos_b if edge < 2 else self.pos_a
        out = self.across(slot, edge, along)
        step = 1 if edge % 2 else -1
        inside = (
            self.core,
            self.pos_a + (step if edge < 2 else 0),
            self.pos_b + (0 if edge < 2 else step),
            slot * EDGES + (edge ^ 1),
        )
        return tuple(mix(self.at_edge[edge], o, i) for o, i in zip(out, inside))

    def corner(self, slot, end_a, end_b):
        step_a, step_b = 2 * end_a - 1, 2 * end_b - 1
        out_a, out_b = self.at_edge[end_a], self.at_edge[2 + end_b]
        by_a = self.across(slot, end_a, self.pos_b + step_b, 1 - end_b)
        by_b = self.across(slot, 2 + end_b, self.pos_a + step_a, 1 - end_a)
        inside = (self.core, self.pos_a + step_a, self.pos_b + step_b, slot * EDGES + 2 * (1 - end_a) + 1 - end_b)
        return tuple(mix(out_a, x, mix(out_b, y, z)) for x, y, z in zip(by_a, by_b, inside))

    def lone(self, end_a, end_b):
        return self.at_edge[end_a] * self.at_edge[2 + end_b]

    def here(self, found):
        return same(found[0], self.core) * same(found[1], self.pos_a) * same(found[2], self.pos_b)

    def can_stay(self, slot, edge):
        for core in range(self.cores):
            other, other_edge, flipped = NEIGHBOURS[core * self.slots + slot][edge]
            if other // self.slots == core:
                for along in range(self.count):
                    place = self.count - 1 - along if flipped else along
                    if on_edge(edge, along, self.count) == on_edge(other_edge, place, self.count):
                        return True
        return False

    def flip(self, slot, edge):
        values = [NEIGHBOURS[core * self.slots + slot][edge][2] for core in range(self.cores)]
        if not any(values):
            return None
        return self.at_edge[edge] * pick(self.core, values)


def roll(x, shift, axis):
    shift = shift % x.shape[axis]
    return x if shift == 0 else pltpu.roll(x, shift, axis)


def kernel(cores, count, tile, height, wind_u, wind_v, sqrt_g, metric_aa, metric_ab, metric_bb, coriolis,
           topography, coef_e, coef_c, tracers, out_h, out_u, out_v, out_q,
           dyn_a, dyn_b, tra_a, tra_b, stat, area, aux, coef, pack, ghost_t, ghost_d, ghost_q,
           *traffic):
    slots = 6 // cores
    fields = tracers.shape[0]
    plan = Plan(lax.axis_index('panel'), lax.axis_index('tx'), lax.axis_index('ty'), cores, count)
    edges = [[plan.edge(s, e) for e in range(EDGES)] for s in range(slots)]
    corners = [[plan.corner(s, k // 2, k % 2) for k in range(EDGES)] for s in range(slots)]
    lone = [plan.lone(k // 2, k % 2) for k in range(EDGES)]
    stays = [[plan.here(edges[s][e]) if plan.can_stay(s, e) else None for e in range(EDGES)] for s in range(slots)]
    lanes = lambda rows: lax.broadcasted_iota(jnp.int32, (rows, LANES), 1)
    lane = lanes(1)
    lane8 = lax.broadcasted_iota(jnp.int32, (8, LANES), 1)
    even8 = lax.broadcasted_iota(jnp.int32, (8, LANES), 0) % 2 == 0
    last_lane = tile - LANES - 1
    inner = pl.ds(TOP, tile)
    one = lambda k: pl.ds(k, 1)

    def where_to(found):
        return {'panel': found[0], 'tx': found[1], 'ty': found[2]}

    of_dyn, of_tra, of_end = (traffic[k::BASE] for k in range(BASE))

    def start(kind, par, index, found, stay=None):
        send, recv, spare, sent, landed = kind

        def away():
            pltpu.make_async_remote_copy(
                src_ref=send.at[par, index], dst_ref=recv.at[par, found[-1]], send_sem=sent.at[par],
                recv_sem=landed.at[par], device_id=where_to(found), device_id_type=pl.DeviceIdType.MESH).start()

        def inside():
            pltpu.make_async_copy(send.at[par, index], recv.at[par, found[-1]], landed.at[par]).start()
            pltpu.make_async_copy(send.at[par, index], spare.at[par, index], sent.at[par]).start()
        if stay is None:
            away()
        else:
            pl.when(stay == 0)(away)
            pl.when(stay == 1)(inside)

    def wait_for(kind, par):
        send, recv, _, sent, landed = kind
        pltpu.make_async_copy(recv.at[par], recv.at[par], landed.at[par]).wait()
        pltpu.make_async_copy(send.at[par], send.at[par], sent.at[par]).wait()

    of_end[1][...] = jnp.zeros_like(of_end[1])
    barrier = pltpu.get_barrier_semaphore()
    expected = 0
    for s in range(slots):
        for e in range(EDGES):
            stay = 0 if stays[s][e] is None else stays[s][e]

            def tell(s=s, e=e):
                pl.semaphore_signal(barrier, inc=1, device_id=where_to(edges[s][e]), device_id_type=pl.DeviceIdType.MESH)
            if stays[s][e] is None:
                tell()
            else:
                pl.when(stay == 0)(tell)
            expected = expected + 1 - stay
        for k in range(EDGES):
            @pl.when(lone[k] == 0)
            def _(s=s, k=k):
                pl.semaphore_signal(barrier, inc=1, device_id=where_to(corners[s][k]), device_id_type=pl.DeviceIdType.MESH)
            expected = expected + 1 - lone[k]

    def swap_pairs(x):
        return jnp.where(even8, roll(x, -1, 0), roll(x, 1, 0))

    def send_all(kind, par):
        for s in range(slots):
            for e in range(EDGES):
                start(kind, par, EDGES * s + e, edges[s][e], stays[s][e])

    def pack_columns(src, count_f, depth, send, par):
        def step(i, carry):
            r0 = pl.multiple_of(ROWSP * i, ROWSP)
            rows = pl.ds(r0 + TOP, ROWSP)
            lane = lanes(ROWSP)
            packed = jnp.zeros((ROWSP, LANES), F32)
            for s in range(slots):
                for f in range(count_f):
                    low = DEPTH * TOP * s + depth * f
                    high = low + TOP
                    x = roll(src(s)[f, 0, rows, :], low, 1)
                    packed = jnp.where((lane >= low) & (lane < low + depth), x, packed)
                    x = roll(src(s)[f, 1, rows, :], high - last_lane + depth - 1, 1)
                    packed = jnp.where((lane >= high) & (lane < high + depth), x, packed)
            pack[pl.ds(r0, ROWSP), :] = packed
            return carry
        lax.fori_loop(0, tile // ROWSP, step, 0)
        turned0 = jnp.transpose(pack[:LANES])
        turned1 = jnp.transpose(pack[LANES:])
        for s in range(slots):
            for side in range(DEPTH):
                g = TOP * (DEPTH * s + side)
                left = turned0[g:g + TOP]
                right = jnp.where(lane8 < tile - LANES, turned1[g:g + TOP], left)
                if side and depth == DEPTH:
                    left, right = swap_pairs(left), swap_pairs(right)
                index = EDGES * s + DEPTH + side
                send[par, index, 0] = left
                send[par, index, 1] = right

    def pack_rows(src, count_f, depth, send, par):
        for s in range(slots):
            for f in range(count_f):
                for d in range(depth):
                    k = one(depth * f + d)
                    send[par, EDGES * s, :, k, :] = src(s)[f, :, one(TOP + d), :]
                    send[par, EDGES * s + 1, :, k, :] = src(s)[f, :, one(tile + TOP - 1 - d), :]

    def send_corners(src, par):
        send = of_end[0]
        for s in range(slots):
            for k in range(EDGES):
                end_a, end_b = divmod(k, DEPTH)
                row = tile + TOP - 1 if end_a else TOP
                at = last_lane if end_b else 0
                for f in range(1, BASE):
                    cell = src(s)[f, end_b, one(row), one(at)]
                    send[par, EDGES * s + k, one(f - 1), :] = jnp.broadcast_to(cell, (1, LANES))
        for s in range(slots):
            for k in range(EDGES):
                found = corners[s][k]
                mine = EDGES * s + k
                start(of_end, par, mine, found[:-1] + (mix(lone[k], mine, found[-1]),), lone[k])

    def unpack(dst, count_f, depth, kind, par, ghosts, turn):
        recv = kind[1]
        wait_for(kind, par)
        ends = {}
        for s in range(slots):
            for e in range(EDGES):
                index = EDGES * s + e
                left, right = recv[par, index, 0], recv[par, index, 1]
                flip = plan.flip(s, e)
                if flip is not None:
                    flipped = (jnp.zeros_like(lane8) + flip) == 1
                    mirror = lane8 ^ last_lane
                    back = jnp.take_along_axis(right, mirror, axis=1)
                    forth = jnp.take_along_axis(left, mirror, axis=1)
                    left, right = jnp.where(flipped, back, left), jnp.where(flipped, forth, right)
                if turn:
                    both = []
                    for lr, x in enumerate((left, right)):
                        stay, down, up = (coef_e[index, lr, k] for k in range(BASE))
                        both.append(stay * x + down * roll(x, DEPTH, 0) + up * roll(x, -DEPTH, 0))
                    left, right = both
                if e < DEPTH:
                    for f in range(count_f):
                        for d in range(depth):
                            k = depth * f + d
                            row = one(tile + TOP + d if e else TOP - 1 - d)
                            dst(s)[f, 0, row, :] = left[k:k + 1]
                            dst(s)[f, 1, row, :] = right[k:k + 1]
                    ends[s, e] = (left, right)
                else:
                    if e == DEPTH and depth == DEPTH:
                        left, right = swap_pairs(left), swap_pairs(right)
                    g = pl.ds(TOP * (DEPTH * s + e - DEPTH), TOP)
                    ghost_t[0, g, :] = jnp.where(lane8 < HALF, left, right)
                    ghost_t[1, g, :] = right
        low = jnp.transpose(ghost_t[0])
        high = jnp.transpose(ghost_t[1])[:tile - LANES]
        for s in range(slots):
            shift = -DEPTH * TOP * s
            ghosts[s, pl.ds(TOP, LANES), :] = roll(low, shift, 1)
            ghosts[s, pl.ds(TOP + LANES, tile - LANES), :] = roll(high, shift, 1)
        return ends

    def unpack_corners(par, ends):
        wait_for(of_end, par)
        for s in range(slots):
            rows = [jnp.zeros((1, LANES), F32)] * DEPTH
            for k in range(EDGES):
                end_a, end_b = divmod(k, DEPTH)
                x = of_end[1][par, EDGES * s + k]
                stay, down, up = (coef_c[EDGES * s + k, j] for j in range(BASE))
                x = stay * x + down * roll(x, 1, 0) + up * roll(x, -1, 0)
                alone = (jnp.zeros_like(lane) + lone[k]) == 1
                edge_row = ends[s, end_a][end_b]
                at = last_lane if end_b else 0
                for f in range(1, BASE):
                    mirrored = jnp.broadcast_to(edge_row[DEPTH * f:DEPTH * f + 1, at:at + 1], (1, LANES))
                    value = jnp.where(alone, mirrored, x[f - 1:f])
                    place = DEPTH * f + (TOP if end_b else 1)
                    rows[end_a] = jnp.where(lane == place, value, rows[end_a])
            ghost_d[s, one(TOP - 1), :] = rows[0]
            ghost_d[s, one(tile + TOP), :] = rows[1]

    def exchanged(left, right):
        lane = lanes(left.shape[0])
        return (jnp.where((lane == HALF) | (lane == HALF + 1), right, left),
                jnp.where((lane == HALF - 1) | (lane == HALF - 2), left, right))

    def with_columns(x, ghosts, low):
        left, right = exchanged(x[0], x[1])
        lane = lanes(left.shape[0])
        left = jnp.where(lane >= LANES - 2, roll(ghosts, LANES - 2 - low, 1), left)
        ghosts = roll(ghosts, tile - LANES - low - 8, 1)
        right = jnp.where((lane == tile - LANES) | (lane == tile - LANES + 1), ghosts, right)
        return jnp.stack([left, right])

    def take(src, dst):
        dst[0, inner, :] = src[:, :LANES]
        dst[1, inner, :] = roll(src[:, tile - LANES:], tile - LANES, 1)

    zero_rows = jnp.zeros((2 * LANES - tile, LANES), F32)
    pack[tile:2 * LANES, :] = zero_rows
    ghost_t[...] = jnp.zeros_like(ghost_t)
    ghost_d[...] = jnp.zeros_like(ghost_d)
    ghost_q[...] = jnp.zeros_like(ghost_q)
    for kind in (of_dyn, of_end):
        kind[0][...] = jnp.zeros_like(kind[0])
    group0 = lambda s: stat.at[s, 0]
    group1 = lambda s: stat.at[s, 1]
    def take_state(s, carry):
        for k, ref in enumerate((sqrt_g, metric_aa, metric_ab)):
            take(ref.at[s], stat.at[s, 0, k])
        for k, ref in enumerate((metric_bb, topography, coriolis)):
            take(ref.at[s], stat.at[s, 1, k])
        for k, ref in enumerate((height, wind_u, wind_v)):
            take(ref.at[s], dyn_a.at[s, k])
        return carry
    lax.fori_loop(0, slots, take_state, 0)
    dyn_of = {0: lambda s: dyn_a.at[s], 1: lambda s: dyn_b.at[s]}
    tra_of = {0: lambda s: tra_a.at[s], 1: lambda s: tra_b.at[s]}
    groups = (DEPTH, group0), (BASE, group1)
    for par, group in groups:
        pack_columns(group, BASE, DEPTH, of_dyn[0], par)
        pack_rows(group, BASE, DEPTH, of_dyn[0], par)
        if par == DEPTH:
            pl.semaphore_wait(barrier, expected)
        send_all(of_dyn, par)

    def pack_dyn(par):
        pack_columns(dyn_of[par], BASE, DEPTH, of_dyn[0], par)
        pack_rows(dyn_of[par], BASE, DEPTH, of_dyn[0], par)
        send_all(of_dyn, par)
        send_corners(dyn_of[par], par)

    def pack_tra(par):
        pack_columns(tra_of[par], fields, 1, of_tra[0], par)
        pack_rows(tra_of[par], fields, 1, of_tra[0], par)
        send_all(of_tra, par)

    pack_dyn(0)
    def take_tracer(t, carry):
        for s in range(slots):
            take(tracers.at[t, s], tra_a.at[s, t])
        return carry
    lax.fori_loop(0, fields, take_tracer, 0)
    pack_tra(0)

    for par, group in groups:
        unpack(group, BASE, DEPTH, of_dyn, par, ghost_d, False)
        def fill_slot(s, carry):
            def fill(i, carry):
                rows = pl.ds(pl.multiple_of(ROWSP * i, ROWSP) + 8, ROWSP)
                g = ghost_d[s, rows, :]
                for f in range(3):
                    group(s)[f, :, rows, :] = with_columns(group(s)[f, :, rows, :], g, 2 * f)
                if par == DEPTH:
                    inverse = 1.0 / group(s)[0, :, rows, :]
                    area[s, 0, :, rows, :] = inverse
                    area[s, 1, :, rows, :] = (-0.5 * TIME_STEP) * inverse
                return carry
            return lax.fori_loop(0, tile // ROWSP, fill, carry)
        lax.fori_loop(0, slots, fill_slot, 0)

    def first_pass(s, now):
        state = dyn_of[now](s)

        def step(i, carry):
            rows = pl.ds(pl.multiple_of(ROWS1 * i, ROWS1), ROWS1)
            g = ghost_d[s, rows, :]
            h, u, v = (with_columns(state[f, :, rows, :], g, 2 * f) for f in range(3))
            state[0, :, rows, :] = h
            state[1, :, rows, :] = u
            state[2, :, rows, :] = v
            jac, gaa, gab = (stat[s, 0, k, :, rows, :] for k in range(3))
            gbb, top = (stat[s, 1, k, :, rows, :] for k in range(2))
            contra_a = gaa * u + gab * v
            contra_b = gab * u + gbb * v
            jh = jac * h
            aux[0, :, rows, :] = GRAVITY * (h + top) + 0.5 * (u * contra_a + v * contra_b)
            aux[1, :, rows, :] = jh * contra_a
            aux[2, :, rows, :] = jh * contra_b
            aux[3, :, rows, :] = contra_a
            aux[4, :, rows, :] = contra_b
            return carry
        lax.fori_loop(0, (tile + 16) // ROWS1, step, 0)

    def second_pass(s, now):
        state, fresh = dyn_of[now](s), dyn_of[1 - now](s)

        def step(i, carry):
            r0 = pl.multiple_of(ROWS2 * i, 8) + 8

            def at(ref, f, shift=0):
                return ref[f, :, pl.ds(r0 + shift, ROWS2), :]
            rows = pl.ds(r0, ROWS2)
            h, u, v = (at(state, f) for f in range(3))
            area_here = area.at[s]
            inv_jac = at(area_here, 0)
            jac = at(stat.at[s, 0], 0)
            mass_a = at(aux, 1)
            plus, minus = mass_a + h, mass_a - h
            flux_e = plus + (at(aux, 1, 1) - at(state, 0, 1))
            flux_w = (at(aux, 1, -1) + at(state, 0, -1)) + minus
            mass_b = at(aux, 2)
            flux_n = (mass_b + h) + roll(mass_b - h, -1, 2)
            flux_s = roll(flux_n, 1, 2)
            total = (flux_e - flux_w) + (flux_n - flux_s)
            h_t = (-0.5) * total * inv_jac
            coef[s, 0, :, rows, :] = 0.5 * total + 4.0
            coef[s, 1, :, rows, :] = 0.5 * flux_e - 1.0
            coef[s, 2, :, rows, :] = -0.5 * flux_w - 1.0
            coef[s, 3, :, rows, :] = 0.5 * flux_n - 1.0
            coef[s, 4, :, rows, :] = -0.5 * flux_s - 1.0
            twelfth = 1.0 / 12.0
            e = at(aux, 0)
            slope_a = (8.0 * (at(aux, 0, 1) - at(aux, 0, -1)) - (at(aux, 0, 2) - at(aux, 0, -2))) * twelfth
            slope_b = (8.0 * (roll(e, -1, 2) - roll(e, 1, 2)) - (roll(e, -2, 2) - roll(e, 2, 2))) * twelfth
            v_e, v_w = at(state, 2, 1), at(state, 2, -1)
            turn_v = (8.0 * (v_e - v_w) - (at(state, 2, 2) - at(state, 2, -2))) * twelfth
            u_n, u_s = roll(u, -1, 2), roll(u, 1, 2)
            turn_u = (8.0 * (u_n - u_s) - (roll(u, -2, 2) - roll(u, 2, 2))) * twelfth
            spin = ((turn_v - turn_u) * inv_jac + at(stat.at[s, 1], 2)) * jac
            pair_u = at(state, 1, 1) + at(state, 1, -1)
            lap_u = (4.0 * (pair_u + (u_n + u_s)) + (roll(pair_u, -1, 2) + roll(pair_u, 1, 2)) - 20.0 * u) * (1.0 / 6.0)
            pair_v = v_e + v_w
            mid_v = 4.0 * v + pair_v
            lap_v = (4.0 * pair_v + (roll(mid_v, -1, 2) + roll(mid_v, 1, 2)) - 20.0 * v) * (1.0 / 6.0)
            u_t = spin * at(aux, 4) - slope_a + WAVE_SPEED * lap_u
            v_t = WAVE_SPEED * lap_v - spin * at(aux, 3) - slope_b
            for f, (x, x_t) in enumerate(((h, h_t), (u, u_t), (v, v_t))):
                new = x + TIME_STEP * x_t
                if now == 1:
                    new = 0.5 * (at(fresh, f) + new)
                fresh[f, :, rows, :] = new
            return carry
        lax.fori_loop(0, tile // ROWS2, step, 0)

    def tracer_pass(s, now):
        state, fresh = tra_of[now](s), tra_of[1 - now](s)

        def step(i, carry):
            r0 = pl.multiple_of(ROWSB * i, 8) + 8
            rows = pl.ds(r0, ROWSB)
            g = ghost_q[s, rows, :]
            mid, east, west, north, south = (coef[s, k, :, rows, :] for k in range(5))
            scale = area[s, 1, :, rows, :]
            lane = lanes(ROWSB)
            for t in range(fields):
                q = state[t, :, rows, :]
                q_e = state[t, :, pl.ds(r0 + 1, ROWSB), :]
                q_w = state[t, :, pl.ds(r0 - 1, ROWSB), :]
                x = jnp.stack(exchanged(q[0], q[1]))
                low = roll(g, -t, 1)
                high = roll(g, last_lane - TOP - t, 1)
                q_n, q_s = roll(x, -1, 2), roll(x, 1, 2)
                q_s = jnp.stack([jnp.where(lane == 0, low, q_s[0]), q_s[1]])
                q_n = jnp.stack([q_n[0], jnp.where(lane == last_lane, high, q_n[1])])
                total = mid * q + (east * q_e + west * q_w) + (north * q_n + south * q_s)
                new = q + scale * total
                if now == 1:
                    new = 0.5 * (fresh[t, :, rows, :] + new)
                fresh[t, :, rows, :] = new
            return carry
        lax.fori_loop(0, tile // ROWSB, step, 0)

    def stage(now, more):
        ends = unpack(dyn_of[now], BASE, DEPTH, of_dyn, now, ghost_d, True)
        unpack_corners(now, ends)

        def cells(s, carry):
            first_pass(s, now)
            second_pass(s, now)
            return carry
        lax.fori_loop(0, slots, cells, 0)

        def forward(send):
            if more is None:
                send(1 - now)
            else:
                pl.when(more)(lambda: send(1 - now))
        forward(pack_dyn)
        unpack(tra_of[now], fields, 1, of_tra, now, ghost_q, False)

        def tracers_of(s, carry):
            tracer_pass(s, now)
            return carry
        lax.fori_loop(0, slots, tracers_of, 0)
        forward(pack_tra)

    def one_step(step_index, carry):
        stage(0, None)
        stage(1, step_index < STEPS - 1)
        return carry

    lax.fori_loop(0, STEPS, one_step, 0)

    def give(src, dst):
        x0, x1 = src[0, inner, :], src[1, inner, :]
        dst[:, :LANES] = jnp.where(lanes(tile) < HALF, x0, x1)
        dst[:, LANES:] = x1[:, :tile - LANES]

    def give_tracer(t, carry):
        for s in range(slots):
            give(tra_a.at[s, t], out_q.at[t, s])
        return carry
    lax.fori_loop(0, fields, give_tracer, 0)

    def give_state(s, carry):
        for k, ref in enumerate((out_h, out_u, out_v)):
            give(dyn_a.at[s, k], ref.at[s])
        return carry
    lax.fori_loop(0, slots, give_state, 0)


def coefficients(rotation, pos_a, pos_b, count, tile):
    slots = rotation.shape[0]
    line = jnp.transpose(rotation, (0, 1, 3, 4, 2)).reshape(slots, 4, 4, rotation.shape[2])
    line = jnp.pad(line, ((0, 0), (0, 0), (0, 0), (2, LANES)))
    along = lambda part, pos: lax.dynamic_slice_in_dim(part, pos * tile, 2 * LANES, axis=3)
    line = jnp.concatenate([along(line[:, 0:2], pos_b), along(line[:, 2:4], pos_a)], axis=1)
    edge = jnp.stack([pos_a == 0, pos_a == count - 1, pos_b == 0, pos_b == count - 1])
    one = jnp.array([1.0, 0.0, 0.0, 1.0], F32)[:, None]
    line = jnp.where(edge[:, None, None], line, one)
    left = jnp.concatenate([line[..., 2:LANES], line[..., 0:2]], axis=-1)
    right = jnp.concatenate([line[..., LANES + 2:LANES + HALF], line[..., HALF:LANES + 2]], axis=-1)
    m = jnp.stack([left, right], axis=2)
    m = m.reshape(slots * 4, 2, 4, LANES)
    zero = jnp.zeros_like(m[:, :, 0])
    unit = jnp.ones_like(zero)
    m00, m01, m10, m11 = (m[:, :, k] for k in range(EDGES))
    stay = jnp.stack([unit, unit, m00, m00, m11, m11, zero, zero], axis=2)
    down = jnp.stack([zero, zero, zero, zero, m10, m10, zero, zero], axis=2)
    up = jnp.stack([zero, zero, m01, m01, zero, zero, zero, zero], axis=2)
    coef_e = jnp.stack([stay, down, up], axis=2)

    before, after = line[..., 1], line[..., tile + 2]
    found = []
    for k in range(EDGES):
        end_a, end_b = k // 2, k % 2
        by_a = (after if end_b else before)[:, end_a]
        by_b = (after if end_a else before)[:, 2 + end_b]
        found.append(jnp.where(edge[end_a], by_a, by_b))
    c = jnp.stack(found, axis=1).reshape(slots * 4, 4)
    zero = jnp.zeros_like(c[:, 0])
    rows = jnp.stack([jnp.stack([c[:, 0], c[:, 3]], -1), jnp.stack([zero, c[:, 2]], -1), jnp.stack([c[:, 1], zero], -1)], axis=1)
    rows = jnp.pad(rows, ((0, 0), (0, 0), (0, 6)))
    return coef_e, jnp.broadcast_to(rows[..., None], rows.shape + (LANES,))


def solution(mesh):
    cores, count = mesh.shape['panel'], mesh.shape['tx']
    slots = 6 // cores

    def body(height, wind_u, wind_v, sqrt_g, metric_aa, metric_ab, metric_bb, coriolis, topography, rotation, tracers):
        tile = height.shape[-1]
        fields = tracers.shape[0]
        coef_e, coef_c = coefficients(rotation, lax.axis_index('tx'), lax.axis_index('ty'), count, tile)
        rows = tile + DEPTH * TOP
        vmem = lambda *shape: pltpu.VMEM(shape, F32)
        blocks = (DEPTH, rows, LANES)
        state = [vmem(slots, count_f, *blocks) for count_f in (BASE, BASE, fields, fields)]
        messages = slots * EDGES
        buffers = [vmem(DEPTH + DEPTH, messages, DEPTH, TOP, LANES), vmem(DEPTH, messages, DEPTH, TOP, LANES),
                   vmem(DEPTH, messages, TOP, LANES)]
        counters = [pltpu.SemaphoreType.DMA((count_p,)) for count_p in (DEPTH + DEPTH, DEPTH, DEPTH)]
        whole = pl.BlockSpec(memory_space=pltpu.VMEM)
        args = (height, wind_u, wind_v, sqrt_g, metric_aa, metric_ab, metric_bb, coriolis, topography, coef_e, coef_c, tracers)
        outs = [jax.ShapeDtypeStruct(x.shape, F32) for x in (height, wind_u, wind_v, tracers)]
        call = pl.pallas_call(
            functools.partial(kernel, cores, count, tile),
            out_shape=outs,
            in_specs=[whole] * len(args),
            out_specs=[whole] * len(outs),
            scratch_shapes=state + [
                vmem(slots, DEPTH, BASE, *blocks), vmem(slots, DEPTH, *blocks),
                vmem(BASE + DEPTH, *blocks), vmem(slots, BASE + DEPTH, *blocks),
                vmem(DEPTH * LANES, LANES), vmem(DEPTH, LANES, LANES), vmem(slots, rows, LANES), vmem(slots, rows, LANES),
            ] + buffers * BASE + counters * DEPTH,
            compiler_params=pltpu.CompilerParams(
                collective_id=0, has_side_effects=True, vmem_limit_bytes=63 << 20),
            name='swe',
        )
        return tuple(call(*args))

    state_spec = P(('member', 'panel'), 'tx', 'ty')
    static_spec = P('panel', 'tx', 'ty')
    tracer_spec = P(None, ('member', 'panel'), 'tx', 'ty')
    in_specs = (state_spec, state_spec, state_spec, static_spec, static_spec, static_spec, static_spec, static_spec, static_spec, P('panel'), tracer_spec)
    out_specs = (state_spec, state_spec, state_spec, tracer_spec)
    return jax.shard_map(body, mesh=mesh, in_specs=in_specs, out_specs=out_specs, check_vma=False)
```

```python
import functools

import jax
import jax.numpy as jnp
from jax import lax
from jax.experimental import pallas as pl
from jax.experimental.pallas import tpu as pltpu
from jax.sharding import PartitionSpec as P

STEPS = 8
TIME_STEP = 0.1
GRAVITY = 1.0
WAVE_SPEED = 1.0
LINKS = (
    '310 100 530 420',
    '010 200 511 410',
    '110 300 521 431',
    '210 000 500 401',
    '331 130 030 231',
    '320 121 221 020',
)
NEIGHBOURS = tuple(tuple(tuple(map(int, link)) for link in row.split()) for row in LINKS)
LANES = 128
HALF = 96
TOP = 8
EDGES = 4
BASE = 3
DEPTH = 2
SPLIT = 32
ROWS1, PARTS1 = 104, 1
ROWS2, PARTS2 = 48, 1
ROWSB, PARTSB = 16, 4
ROWSP = 96
F32 = jnp.float32


def pick(index, values):
    if all(value is values[0] for value in values):
        return values[0]
    total = 0
    for place, value in enumerate(values):
        total = total + same(index, place) * value
    return total


def same(x, y):
    return 1 - lax.min((x - y) * (x - y), 1)


def mix(cond, yes, no):
    return cond * yes + (1 - cond) * no


def on_edge(edge, along, count):
    if edge == 0:
        return 0, along
    if edge == 1:
        return count - 1, along
    if edge == 2:
        return along, 0
    return along, count - 1


class Plan:
    def __init__(self, core, pos_a, pos_b, cores, count):
        self.core, self.pos_a, self.pos_b = core, pos_a, pos_b
        self.cores, self.count = cores, count
        self.slots = 6 // cores
        first = lambda x: 1 - lax.div(x + count - 1, count)
        last = lambda x: lax.div(x + 1, count)
        self.at_edge = (first(pos_a), last(pos_a), first(pos_b), last(pos_b))

    def across(self, slot, edge, along, side=None):
        found = []
        for core in range(self.cores):
            other, other_edge, flipped = NEIGHBOURS[core * self.slots + slot][edge]
            place = self.count - 1 - along if flipped else along
            tile_a, tile_b = on_edge(other_edge, place, self.count)
            if side is None:
                index = (other % self.slots) * EDGES + other_edge
            else:
                end = 1 - side if flipped else side
                if other_edge < 2:
                    index = (other % self.slots) * EDGES + 2 * other_edge + end
                else:
                    index = (other % self.slots) * EDGES + 2 * end + other_edge - 2
            found.append((other // self.slots, tile_a, tile_b, index))
        return tuple(pick(self.core, [entry[k] for entry in found]) for k in range(EDGES))

    def edge(self, slot, edge):
        along = self.pos_b if edge < 2 else self.pos_a
        out = self.across(slot, edge, along)
        step = 1 if edge % 2 else -1
        inside = (
            self.core,
            self.pos_a + (step if edge < 2 else 0),
            self.pos_b + (0 if edge < 2 else step),
            slot * EDGES + (edge ^ 1),
        )
        return tuple(mix(self.at_edge[edge], o, i) for o, i in zip(out, inside))

    def corner(self, slot, end_a, end_b):
        step_a, step_b = 2 * end_a - 1, 2 * end_b - 1
        out_a, out_b = self.at_edge[end_a], self.at_edge[2 + end_b]
        by_a = self.across(slot, end_a, self.pos_b + step_b, 1 - end_b)
        by_b = self.across(slot, 2 + end_b, self.pos_a + step_a, 1 - end_a)
        inside = (self.core, self.pos_a + step_a, self.pos_b + step_b, slot * EDGES + 2 * (1 - end_a) + 1 - end_b)
        return tuple(mix(out_a, x, mix(out_b, y, z)) for x, y, z in zip(by_a, by_b, inside))

    def lone(self, end_a, end_b):
        return self.at_edge[end_a] * self.at_edge[2 + end_b]

    def here(self, found):
        return same(found[0], self.core) * same(found[1], self.pos_a) * same(found[2], self.pos_b)

    def can_stay(self, slot, edge):
        for core in range(self.cores):
            other, other_edge, flipped = NEIGHBOURS[core * self.slots + slot][edge]
            if other // self.slots == core:
                for along in range(self.count):
                    place = self.count - 1 - along if flipped else along
                    if on_edge(edge, along, self.count) == on_edge(other_edge, place, self.count):
                        return True
        return False

    def flip(self, slot, edge):
        values = [NEIGHBOURS[core * self.slots + slot][edge][2] for core in range(self.cores)]
        if not any(values):
            return None
        return self.at_edge[edge] * pick(self.core, values)


def roll(x, shift, axis):
    shift = shift % x.shape[axis]
    return x if shift == 0 else pltpu.roll(x, shift, axis)


def kernel(cores, count, tile, height, wind_u, wind_v, sqrt_g, metric_aa, metric_ab, metric_bb, coriolis,
           topography, coef_e, coef_c, tracers, out_h, out_u, out_v, out_q,
           dyn_a, dyn_b, tra_a, tra_b, stat, area, aux, coef, pack, ghost_t, ghost_d, ghost_q,
           *traffic):
    slots = 6 // cores
    fields = tracers.shape[0]
    plan = Plan(lax.axis_index('panel'), lax.axis_index('tx'), lax.axis_index('ty'), cores, count)
    edges = [[plan.edge(s, e) for e in range(EDGES)] for s in range(slots)]
    corners = [[plan.corner(s, k // 2, k % 2) for k in range(EDGES)] for s in range(slots)]
    lone = [plan.lone(k // 2, k % 2) for k in range(EDGES)]
    stays = [[plan.here(edges[s][e]) if plan.can_stay(s, e) else None for e in range(EDGES)] for s in range(slots)]
    lanes = lambda rows: lax.broadcasted_iota(jnp.int32, (rows, LANES), 1)
    lane = lanes(1)
    lane8 = lax.broadcasted_iota(jnp.int32, (8, LANES), 1)
    even8 = lax.broadcasted_iota(jnp.int32, (8, LANES), 0) % 2 == 0
    last_lane = tile - LANES - 1
    inner = pl.ds(TOP, tile)
    one = lambda k: pl.ds(k, 1)

    def where_to(found):
        return {'panel': found[0], 'tx': found[1], 'ty': found[2]}

    of_dyn, of_tra, of_end = (traffic[k::BASE] for k in range(BASE))

    def start(kind, par, index, found, stay=None):
        send, recv, spare, sent, landed = kind

        def away():
            pltpu.make_async_remote_copy(
                src_ref=send.at[par, index], dst_ref=recv.at[par, found[-1]], send_sem=sent.at[par],
                recv_sem=landed.at[par], device_id=where_to(found), device_id_type=pl.DeviceIdType.MESH).start()

        def inside():
            pltpu.make_async_copy(send.at[par, index], recv.at[par, found[-1]], landed.at[par]).start()
            pltpu.make_async_copy(send.at[par, index], spare.at[par, index], sent.at[par]).start()
        if stay is None:
            away()
        else:
            pl.when(stay == 0)(away)
            pl.when(stay == 1)(inside)

    def wait_for(kind, par):
        send, recv, _, sent, landed = kind
        pltpu.make_async_copy(recv.at[par], recv.at[par], landed.at[par]).wait()
        pltpu.make_async_copy(send.at[par], send.at[par], sent.at[par]).wait()

    of_end[1][...] = jnp.zeros_like(of_end[1])
    barrier = pltpu.get_barrier_semaphore()
    expected = 0
    for s in range(slots):
        for e in range(EDGES):
            stay = 0 if stays[s][e] is None else stays[s][e]

            def tell(s=s, e=e):
                pl.semaphore_signal(barrier, inc=1, device_id=where_to(edges[s][e]), device_id_type=pl.DeviceIdType.MESH)
            if stays[s][e] is None:
                tell()
            else:
                pl.when(stay == 0)(tell)
            expected = expected + 1 - stay
        for k in range(EDGES):
            @pl.when(lone[k] == 0)
            def _(s=s, k=k):
                pl.semaphore_signal(barrier, inc=1, device_id=where_to(corners[s][k]), device_id_type=pl.DeviceIdType.MESH)
            expected = expected + 1 - lone[k]

    def swap_pairs(x):
        return jnp.where(even8, roll(x, -1, 0), roll(x, 1, 0))

    def send_all(kind, par):
        for s in range(slots):
            for e in range(EDGES):
                start(kind, par, EDGES * s + e, edges[s][e], stays[s][e])

    def pack_columns(src, count_f, depth, send, par):
        def step(i, carry):
            r0 = pl.multiple_of(ROWSP * i, ROWSP)
            rows = pl.ds(r0 + TOP, ROWSP)
            lane = lanes(ROWSP)
            packed = jnp.zeros((ROWSP, LANES), F32)
            for s in range(slots):
                for f in range(count_f):
                    low = TOP * s + depth * f
                    high = low + tile - LANES - depth
                    x = roll(jnp.where(lane < TOP, src(s)[f, 0, rows, :], src(s)[f, 1, rows, :]), low, 1)
                    own = (lane >= low) & (lane < low + depth) | (lane >= high) & (lane < high + depth)
                    packed = jnp.where(own, x, packed)
            packed = jnp.where(lane < SPLIT, packed, roll(packed, depth, 1))
            pack[pl.ds(r0, ROWSP), :] = packed
            return carry
        lax.fori_loop(0, tile // ROWSP, step, 0)
        turned0 = jnp.transpose(pack[:LANES])
        turned1 = jnp.transpose(pack[LANES:])
        for s in range(slots):
            for side in range(DEPTH):
                g = TOP * s + (tile - LANES) * side
                left = turned0[g:g + TOP]
                right = jnp.where(lane8 < tile - LANES, turned1[g:g + TOP], left)
                if side and depth == DEPTH:
                    left, right = swap_pairs(left), swap_pairs(right)
                index = EDGES * s + DEPTH + side
                send[par, index, 0] = left
                send[par, index, 1] = right

    def pack_rows(src, count_f, depth, send, par):
        for s in range(slots):
            for f in range(count_f):
                for d in range(depth):
                    k = one(depth * f + d)
                    send[par, EDGES * s, :, k, :] = src(s)[f, :, one(TOP + d), :]
                    send[par, EDGES * s + 1, :, k, :] = src(s)[f, :, one(tile + TOP - 1 - d), :]

    def send_corners(src, par):
        send = of_end[0]
        for s in range(slots):
            for k in range(EDGES):
                end_a, end_b = divmod(k, DEPTH)
                row = tile + TOP - 1 if end_a else TOP
                at = last_lane if end_b else 0
                for f in range(1, BASE):
                    cell = src(s)[f, end_b, one(row), one(at)]
                    send[par, EDGES * s + k, one(f - 1), :] = jnp.broadcast_to(cell, (1, LANES))
        for s in range(slots):
            for k in range(EDGES):
                found = corners[s][k]
                mine = EDGES * s + k
                start(of_end, par, mine, found[:-1] + (mix(lone[k], mine, found[-1]),), lone[k])

    def unpack(dst, count_f, depth, kind, par, ghosts, lean, turn):
        recv = kind[1]
        wait_for(kind, par)
        ends = {}
        for s in range(slots):
            for e in range(EDGES):
                index = EDGES * s + e
                left, right = recv[par, index, 0], recv[par, index, 1]
                flip = plan.flip(s, e)
                if flip is not None:
                    flipped = (jnp.zeros_like(lane8) + flip) == 1
                    mirror = lane8 ^ last_lane
                    back = jnp.take_along_axis(right, mirror, axis=1)
                    forth = jnp.take_along_axis(left, mirror, axis=1)
                    left, right = jnp.where(flipped, back, left), jnp.where(flipped, forth, right)
                if turn:
                    both = []
                    for lr, x in enumerate((left, right)):
                        stay, down, up = (coef_e[index, lr, k] for k in range(BASE))
                        both.append(stay * x + down * roll(x, DEPTH, 0) + up * roll(x, -DEPTH, 0))
                    left, right = both
                if e < DEPTH:
                    for f in range(count_f):
                        for d in range(depth):
                            k = depth * f + d
                            row = one(tile + TOP + d if e else TOP - 1 - d)
                            dst(s)[f, 0, row, :] = left[k:k + 1]
                            dst(s)[f, 1, row, :] = right[k:k + 1]
                    ends[s, e] = (left, right)
                else:
                    if e == DEPTH and depth == DEPTH:
                        left, right = swap_pairs(left), swap_pairs(right)
                    g = pl.ds(TOP * s + (tile - LANES) * (e - DEPTH), TOP)
                    ghost_t[0, g, :] = jnp.where(lane8 < HALF, left, right)
                    ghost_t[1, g, :] = right
        low = jnp.transpose(ghost_t[0])
        high = jnp.transpose(ghost_t[1])[:tile - LANES]
        low = jnp.where(lanes(LANES) < SPLIT, low, roll(low, lean, 1))
        high = jnp.where(lanes(tile - LANES) < SPLIT, high, roll(high, lean, 1))
        for s in range(slots):
            shift = -TOP * s
            ghosts[s, pl.ds(TOP, LANES), :] = roll(low, shift, 1)
            ghosts[s, pl.ds(TOP + LANES, tile - LANES), :] = roll(high, shift, 1)
        return ends

    def unpack_corners(par, ends):
        wait_for(of_end, par)
        for s in range(slots):
            rows = [jnp.zeros((1, LANES), F32)] * DEPTH
            for k in range(EDGES):
                end_a, end_b = divmod(k, DEPTH)
                x = of_end[1][par, EDGES * s + k]
                stay, down, up = (coef_c[EDGES * s + k, j] for j in range(BASE))
                x = stay * x + down * roll(x, 1, 0) + up * roll(x, -1, 0)
                alone = (jnp.zeros_like(lane) + lone[k]) == 1
                edge_row = ends[s, end_a][end_b]
                at = last_lane if end_b else 0
                for f in range(1, BASE):
                    mirrored = jnp.broadcast_to(edge_row[DEPTH * f:DEPTH * f + 1, at:at + 1], (1, LANES))
                    value = jnp.where(alone, mirrored, x[f - 1:f])
                    place = DEPTH * f + (tile - LANES + DEPTH if end_b else 1)
                    rows[end_a] = jnp.where(lane == place, value, rows[end_a])
            ghost_d[s, one(TOP - 1), :] = rows[0]
            ghost_d[s, one(tile + TOP), :] = rows[1]

    def exchanged(left, right):
        lane = lanes(left.shape[0])
        return (jnp.where((lane == HALF) | (lane == HALF + 1), right, left),
                jnp.where((lane == HALF - 1) | (lane == HALF - 2), left, right))

    def with_columns(x, ghosts, low):
        left, right = exchanged(x[0], x[1])
        lane = lanes(left.shape[0])
        ghosts = roll(ghosts, -DEPTH - low, 1)
        left = jnp.where(lane >= LANES - DEPTH, ghosts, left)
        right = jnp.where((lane == tile - LANES) | (lane == tile - LANES + 1), ghosts, right)
        return jnp.stack([left, right])

    def take(src, dst):
        dst[0, inner, :] = src[:, :LANES]
        dst[1, inner, :] = roll(src[:, tile - LANES:], tile - LANES, 1)

    zero_rows = jnp.zeros((2 * LANES - tile, LANES), F32)
    pack[tile:2 * LANES, :] = zero_rows
    ghost_t[...] = jnp.zeros_like(ghost_t)
    ghost_d[...] = jnp.zeros_like(ghost_d)
    ghost_q[...] = jnp.zeros_like(ghost_q)
    for kind in (of_dyn, of_end):
        kind[0][...] = jnp.zeros_like(kind[0])
    group0 = lambda s: stat.at[s, 0]
    group1 = lambda s: stat.at[s, 1]
    def take_state(s, carry):
        for k, ref in enumerate((sqrt_g, metric_aa, metric_ab)):
            take(ref.at[s], stat.at[s, 0, k])
        for k, ref in enumerate((metric_bb, topography, coriolis)):
            take(ref.at[s], stat.at[s, 1, k])
        for k, ref in enumerate((height, wind_u, wind_v)):
            take(ref.at[s], dyn_a.at[s, k])
        return carry
    lax.fori_loop(0, slots, take_state, 0)
    dyn_of = {0: lambda s: dyn_a.at[s], 1: lambda s: dyn_b.at[s]}
    tra_of = {0: lambda s: tra_a.at[s], 1: lambda s: tra_b.at[s]}
    groups = (DEPTH, group0), (BASE, group1)
    for par, group in groups:
        pack_columns(group, BASE, DEPTH, of_dyn[0], par)
        pack_rows(group, BASE, DEPTH, of_dyn[0], par)
        if par == DEPTH:
            pl.semaphore_wait(barrier, expected)
        send_all(of_dyn, par)

    def pack_dyn(par):
        pack_columns(dyn_of[par], BASE, DEPTH, of_dyn[0], par)
        pack_rows(dyn_of[par], BASE, DEPTH, of_dyn[0], par)
        send_all(of_dyn, par)
        send_corners(dyn_of[par], par)

    def pack_tra(par):
        pack_columns(tra_of[par], fields, 1, of_tra[0], par)
        pack_rows(tra_of[par], fields, 1, of_tra[0], par)
        send_all(of_tra, par)

    pack_dyn(0)
    def take_tracer(t, carry):
        for s in range(slots):
            take(tracers.at[t, s], tra_a.at[s, t])
        return carry
    lax.fori_loop(0, fields, take_tracer, 0)
    pack_tra(0)

    for par, group in groups:
        unpack(group, BASE, DEPTH, of_dyn, par, ghost_d, DEPTH, False)
        def fill_slot(s, carry):
            def fill(i, carry):
                rows = pl.ds(pl.multiple_of(ROWSP * i, ROWSP) + 8, ROWSP)
                g = ghost_d[s, rows, :]
                for f in range(3):
                    group(s)[f, :, rows, :] = with_columns(group(s)[f, :, rows, :], g, 2 * f)
                if par == DEPTH:
                    inverse = 1.0 / group(s)[0, :, rows, :]
                    area[s, 0, :, rows, :] = inverse
                    area[s, 1, :, rows, :] = (-0.5 * TIME_STEP) * inverse
                return carry
            return lax.fori_loop(0, tile // ROWSP, fill, carry)
        lax.fori_loop(0, slots, fill_slot, 0)

    def by_blocks(part, total, count_r, count_p):
        def step(i, carry):
            for k in range(count_p):
                part(pl.multiple_of(count_r * count_p * i, TOP) + count_r * k)
            return carry
        lax.fori_loop(0, total // (count_r * count_p), step, 0)

    def first_pass(s, now):
        state = dyn_of[now](s)

        def part(r0):
            rows = pl.ds(r0, ROWS1)
            g = ghost_d[s, rows, :]
            h, u, v = (with_columns(state[f, :, rows, :], g, 2 * f) for f in range(3))
            state[0, :, rows, :] = h
            state[1, :, rows, :] = u
            state[2, :, rows, :] = v
            jac, gaa, gab = (stat[s, 0, k, :, rows, :] for k in range(3))
            gbb, top = (stat[s, 1, k, :, rows, :] for k in range(2))
            contra_a = gaa * u + gab * v
            contra_b = gab * u + gbb * v
            jh = jac * h
            aux[0, :, rows, :] = GRAVITY * (h + top) + 0.5 * (u * contra_a + v * contra_b)
            aux[1, :, rows, :] = jh * contra_a
            aux[2, :, rows, :] = jh * contra_b
            aux[3, :, rows, :] = contra_a
            aux[4, :, rows, :] = contra_b
        by_blocks(part, tile + DEPTH * TOP, ROWS1, PARTS1)

    def second_pass(s, now):
        state, fresh = dyn_of[now](s), dyn_of[1 - now](s)

        def part(r0):
            r0 = r0 + TOP

            def at(ref, f, shift=0):
                return ref[f, :, pl.ds(r0 + shift, ROWS2), :]
            rows = pl.ds(r0, ROWS2)
            h, u, v = (at(state, f) for f in range(3))
            area_here = area.at[s]
            inv_jac = at(area_here, 0)
            jac = at(stat.at[s, 0], 0)
            mass_a = at(aux, 1)
            plus, minus = mass_a + h, mass_a - h
            flux_e = plus + (at(aux, 1, 1) - at(state, 0, 1))
            flux_w = (at(aux, 1, -1) + at(state, 0, -1)) + minus
            mass_b = at(aux, 2)
            plus_b, minus_b = mass_b + h, mass_b - h
            flux_n = plus_b + roll(minus_b, -1, 2)
            flux_s = roll(plus_b, 1, 2) + minus_b
            total = (flux_e - flux_w) + (flux_n - flux_s)
            h_t = (-0.5) * total * inv_jac
            coef[s, 0, :, rows, :] = 0.5 * total + 4.0
            coef[s, 1, :, rows, :] = 0.5 * flux_e - 1.0
            coef[s, 2, :, rows, :] = -0.5 * flux_w - 1.0
            coef[s, 3, :, rows, :] = 0.5 * flux_n - 1.0
            coef[s, 4, :, rows, :] = -0.5 * flux_s - 1.0
            twelfth = 1.0 / 12.0
            e = at(aux, 0)
            slope_a = (8.0 * (at(aux, 0, 1) - at(aux, 0, -1)) - (at(aux, 0, 2) - at(aux, 0, -2))) * twelfth
            slope_b = (8.0 * (roll(e, -1, 2) - roll(e, 1, 2)) - (roll(e, -2, 2) - roll(e, 2, 2))) * twelfth
            v_e, v_w = at(state, 2, 1), at(state, 2, -1)
            turn_v = (8.0 * (v_e - v_w) - (at(state, 2, 2) - at(state, 2, -2))) * twelfth
            u_n, u_s = roll(u, -1, 2), roll(u, 1, 2)
            turn_u = (8.0 * (u_n - u_s) - (roll(u, -2, 2) - roll(u, 2, 2))) * twelfth
            spin = ((turn_v - turn_u) * inv_jac + at(stat.at[s, 1], 2)) * jac
            pair_u = at(state, 1, 1) + at(state, 1, -1)
            lap_u = (4.0 * (pair_u + (u_n + u_s)) + (roll(pair_u, -1, 2) + roll(pair_u, 1, 2)) - 20.0 * u) * (1.0 / 6.0)
            pair_v = v_e + v_w
            mid_v = 4.0 * v + pair_v
            lap_v = (4.0 * pair_v + (roll(mid_v, -1, 2) + roll(mid_v, 1, 2)) - 20.0 * v) * (1.0 / 6.0)
            u_t = spin * at(aux, 4) - slope_a + WAVE_SPEED * lap_u
            v_t = WAVE_SPEED * lap_v - spin * at(aux, 3) - slope_b
            for f, (x, x_t) in enumerate(((h, h_t), (u, u_t), (v, v_t))):
                new = x + TIME_STEP * x_t
                if now == 1:
                    new = 0.5 * (at(fresh, f) + new)
                fresh[f, :, rows, :] = new
        by_blocks(part, tile, ROWS2, PARTS2)

    def tracer_pass(s, now):
        state, fresh = tra_of[now](s), tra_of[1 - now](s)

        def part(r0):
            r0 = r0 + TOP
            rows = pl.ds(r0, ROWSB)
            g = ghost_q[s, rows, :]
            mid, east, west, north, south = (coef[s, k, :, rows, :] for k in range(5))
            scale = area[s, 1, :, rows, :]
            lane = lanes(ROWSB)
            for t in range(fields):
                q = state[t, :, rows, :]
                q_e = state[t, :, pl.ds(r0 + 1, ROWSB), :]
                q_w = state[t, :, pl.ds(r0 - 1, ROWSB), :]
                x = jnp.stack(exchanged(q[0], q[1]))
                ghost = roll(g, -t, 1)
                q_n, q_s = roll(x, -1, 2), roll(x, 1, 2)
                q_s = jnp.stack([jnp.where(lane == 0, ghost, q_s[0]), q_s[1]])
                q_n = jnp.stack([q_n[0], jnp.where(lane == last_lane, ghost, q_n[1])])
                total = mid * q + (east * q_e + west * q_w) + (north * q_n + south * q_s)
                new = q + scale * total
                if now == 1:
                    new = 0.5 * (fresh[t, :, rows, :] + new)
                fresh[t, :, rows, :] = new
        by_blocks(part, tile, ROWSB, PARTSB)

    def stage(now, more):
        ends = unpack(dyn_of[now], BASE, DEPTH, of_dyn, now, ghost_d, DEPTH, True)
        unpack_corners(now, ends)

        def cells(s, carry):
            first_pass(s, now)
            second_pass(s, now)
            return carry
        lax.fori_loop(0, slots, cells, 0)

        def forward(send):
            if more is None:
                send(1 - now)
            else:
                pl.when(more)(lambda: send(1 - now))
        forward(pack_dyn)
        unpack(tra_of[now], fields, 1, of_tra, now, ghost_q, -1, False)

        def tracers_of(s, carry):
            tracer_pass(s, now)
            return carry
        lax.fori_loop(0, slots, tracers_of, 0)
        forward(pack_tra)

    def one_step(step_index, carry):
        stage(0, None)
        stage(1, step_index < STEPS - 1)
        return carry

    lax.fori_loop(0, STEPS, one_step, 0)

    def give(src, dst):
        x0, x1 = src[0, inner, :], src[1, inner, :]
        dst[:, :LANES] = jnp.where(lanes(tile) < HALF, x0, x1)
        dst[:, LANES:] = x1[:, :tile - LANES]

    def give_tracer(t, carry):
        for s in range(slots):
            give(tra_a.at[s, t], out_q.at[t, s])
        return carry
    lax.fori_loop(0, fields, give_tracer, 0)

    def give_state(s, carry):
        for k, ref in enumerate((out_h, out_u, out_v)):
            give(dyn_a.at[s, k], ref.at[s])
        return carry
    lax.fori_loop(0, slots, give_state, 0)


def coefficients(rotation, pos_a, pos_b, count, tile):
    slots = rotation.shape[0]
    line = jnp.transpose(rotation, (0, 1, 3, 4, 2)).reshape(slots, 4, 4, rotation.shape[2])
    line = jnp.pad(line, ((0, 0), (0, 0), (0, 0), (2, LANES)))
    along = lambda part, pos: lax.dynamic_slice_in_dim(part, pos * tile, 2 * LANES, axis=3)
    line = jnp.concatenate([along(line[:, 0:2], pos_b), along(line[:, 2:4], pos_a)], axis=1)
    edge = jnp.stack([pos_a == 0, pos_a == count - 1, pos_b == 0, pos_b == count - 1])
    one = jnp.array([1.0, 0.0, 0.0, 1.0], F32)[:, None]
    line = jnp.where(edge[:, None, None], line, one)
    left = jnp.concatenate([line[..., 2:LANES], line[..., 0:2]], axis=-1)
    right = jnp.concatenate([line[..., LANES + 2:LANES + HALF], line[..., HALF:LANES + 2]], axis=-1)
    m = jnp.stack([left, right], axis=2)
    m = m.reshape(slots * 4, 2, 4, LANES)
    zero = jnp.zeros_like(m[:, :, 0])
    unit = jnp.ones_like(zero)
    m00, m01, m10, m11 = (m[:, :, k] for k in range(EDGES))
    stay = jnp.stack([unit, unit, m00, m00, m11, m11, zero, zero], axis=2)
    down = jnp.stack([zero, zero, zero, zero, m10, m10, zero, zero], axis=2)
    up = jnp.stack([zero, zero, m01, m01, zero, zero, zero, zero], axis=2)
    coef_e = jnp.stack([stay, down, up], axis=2)

    before, after = line[..., 1], line[..., tile + 2]
    found = []
    for k in range(EDGES):
        end_a, end_b = k // 2, k % 2
        by_a = (after if end_b else before)[:, end_a]
        by_b = (after if end_a else before)[:, 2 + end_b]
        found.append(jnp.where(edge[end_a], by_a, by_b))
    c = jnp.stack(found, axis=1).reshape(slots * 4, 4)
    zero = jnp.zeros_like(c[:, 0])
    rows = jnp.stack([jnp.stack([c[:, 0], c[:, 3]], -1), jnp.stack([zero, c[:, 2]], -1), jnp.stack([c[:, 1], zero], -1)], axis=1)
    rows = jnp.pad(rows, ((0, 0), (0, 0), (0, 6)))
    return coef_e, jnp.broadcast_to(rows[..., None], rows.shape + (LANES,))


def solution(mesh):
    cores, count = mesh.shape['panel'], mesh.shape['tx']
    slots = 6 // cores

    def body(height, wind_u, wind_v, sqrt_g, metric_aa, metric_ab, metric_bb, coriolis, topography, rotation, tracers):
        tile = height.shape[-1]
        fields = tracers.shape[0]
        coef_e, coef_c = coefficients(rotation, lax.axis_index('tx'), lax.axis_index('ty'), count, tile)
        rows = tile + DEPTH * TOP
        vmem = lambda *shape: pltpu.VMEM(shape, F32)
        blocks = (DEPTH, rows, LANES)
        state = [vmem(slots, count_f, *blocks) for count_f in (BASE, BASE, fields, fields)]
        messages = slots * EDGES
        buffers = [vmem(DEPTH + DEPTH, messages, DEPTH, TOP, LANES), vmem(DEPTH, messages, DEPTH, TOP, LANES),
                   vmem(DEPTH, messages, TOP, LANES)]
        counters = [pltpu.SemaphoreType.DMA((count_p,)) for count_p in (DEPTH + DEPTH, DEPTH, DEPTH)]
        whole = pl.BlockSpec(memory_space=pltpu.VMEM)
        args = (height, wind_u, wind_v, sqrt_g, metric_aa, metric_ab, metric_bb, coriolis, topography, coef_e, coef_c, tracers)
        outs = [jax.ShapeDtypeStruct(x.shape, F32) for x in (height, wind_u, wind_v, tracers)]
        call = pl.pallas_call(
            functools.partial(kernel, cores, count, tile),
            out_shape=outs,
            in_specs=[whole] * len(args),
            out_specs=[whole] * len(outs),
            scratch_shapes=state + [
                vmem(slots, DEPTH, BASE, *blocks), vmem(slots, DEPTH, *blocks),
                vmem(BASE + DEPTH, *blocks), vmem(slots, BASE + DEPTH, *blocks),
                vmem(DEPTH * LANES, LANES), vmem(DEPTH, LANES, LANES), vmem(slots, rows, LANES), vmem(slots, rows, LANES),
            ] + buffers * BASE + counters * DEPTH,
            compiler_params=pltpu.CompilerParams(
                collective_id=0, has_side_effects=True, vmem_limit_bytes=63 << 20),
            name='swe',
        )
        return tuple(call(*args))

    state_spec = P(('member', 'panel'), 'tx', 'ty')
    static_spec = P('panel', 'tx', 'ty')
    tracer_spec = P(None, ('member', 'panel'), 'tx', 'ty')
    in_specs = (state_spec, state_spec, state_spec, static_spec, static_spec, static_spec, static_spec, static_spec, static_spec, P('panel'), tracer_spec)
    out_specs = (state_spec, state_spec, state_spec, tracer_spec)
    return jax.shard_map(body, mesh=mesh, in_specs=in_specs, out_specs=out_specs, check_vma=False)
```

```python
import functools

import jax
import jax.numpy as jnp
from jax import lax
from jax.experimental import pallas as pl
from jax.experimental.pallas import tpu as pltpu
from jax.sharding import PartitionSpec as P

STEPS = 8
TIME_STEP = 0.1
GRAVITY = 1.0
WAVE_SPEED = 1.0
LINKS = (
    '310 100 530 420',
    '010 200 511 410',
    '110 300 521 431',
    '210 000 500 401',
    '331 130 030 231',
    '320 121 221 020',
)
NEIGHBOURS = tuple(tuple(tuple(map(int, link)) for link in row.split()) for row in LINKS)
LANES = 128
HALF = 96
TOP = 8
EDGES = 4
BASE = 3
DEPTH = 2
SPLIT = 32
ROWS1, PARTS1 = 104, 1
ROWS2, PARTS2 = 48, 1
ROWSB, PARTSB = 16, 4
ROWSP = 96
F32 = jnp.float32


def pick(index, values):
    if all(value is values[0] for value in values):
        return values[0]
    total = 0
    for place, value in enumerate(values):
        total = total + same(index, place) * value
    return total


def same(x, y):
    return 1 - lax.min((x - y) * (x - y), 1)


def mix(cond, yes, no):
    return cond * yes + (1 - cond) * no


def on_edge(edge, along, count):
    if edge == 0:
        return 0, along
    if edge == 1:
        return count - 1, along
    if edge == 2:
        return along, 0
    return along, count - 1


class Plan:
    def __init__(self, core, pos_a, pos_b, cores, count):
        self.core, self.pos_a, self.pos_b = core, pos_a, pos_b
        self.cores, self.count = cores, count
        self.slots = 6 // cores
        first = lambda x: 1 - lax.div(x + count - 1, count)
        last = lambda x: lax.div(x + 1, count)
        self.at_edge = (first(pos_a), last(pos_a), first(pos_b), last(pos_b))

    def across(self, slot, edge, along, side=None):
        found = []
        for core in range(self.cores):
            other, other_edge, flipped = NEIGHBOURS[core * self.slots + slot][edge]
            place = self.count - 1 - along if flipped else along
            tile_a, tile_b = on_edge(other_edge, place, self.count)
            if side is None:
                index = (other % self.slots) * EDGES + other_edge
            else:
                end = 1 - side if flipped else side
                if other_edge < 2:
                    index = (other % self.slots) * EDGES + 2 * other_edge + end
                else:
                    index = (other % self.slots) * EDGES + 2 * end + other_edge - 2
            found.append((other // self.slots, tile_a, tile_b, index))
        return tuple(pick(self.core, [entry[k] for entry in found]) for k in range(EDGES))

    def edge(self, slot, edge):
        along = self.pos_b if edge < 2 else self.pos_a
        out = self.across(slot, edge, along)
        step = 1 if edge % 2 else -1
        inside = (
            self.core,
            self.pos_a + (step if edge < 2 else 0),
            self.pos_b + (0 if edge < 2 else step),
            slot * EDGES + (edge ^ 1),
        )
        return tuple(mix(self.at_edge[edge], o, i) for o, i in zip(out, inside))

    def corner(self, slot, end_a, end_b):
        step_a, step_b = 2 * end_a - 1, 2 * end_b - 1
        out_a, out_b = self.at_edge[end_a], self.at_edge[2 + end_b]
        by_a = self.across(slot, end_a, self.pos_b + step_b, 1 - end_b)
        by_b = self.across(slot, 2 + end_b, self.pos_a + step_a, 1 - end_a)
        inside = (self.core, self.pos_a + step_a, self.pos_b + step_b, slot * EDGES + 2 * (1 - end_a) + 1 - end_b)
        return tuple(mix(out_a, x, mix(out_b, y, z)) for x, y, z in zip(by_a, by_b, inside))

    def lone(self, end_a, end_b):
        return self.at_edge[end_a] * self.at_edge[2 + end_b]

    def here(self, found):
        return same(found[0], self.core) * same(found[1], self.pos_a) * same(found[2], self.pos_b)

    def can_stay(self, slot, edge):
        for core in range(self.cores):
            other, other_edge, flipped = NEIGHBOURS[core * self.slots + slot][edge]
            if other // self.slots == core:
                for along in range(self.count):
                    place = self.count - 1 - along if flipped else along
                    if on_edge(edge, along, self.count) == on_edge(other_edge, place, self.count):
                        return True
        return False

    def flip(self, slot, edge):
        values = [NEIGHBOURS[core * self.slots + slot][edge][2] for core in range(self.cores)]
        if not any(values):
            return None
        return self.at_edge[edge] * pick(self.core, values)


def roll(x, shift, axis):
    shift = shift % x.shape[axis]
    return x if shift == 0 else pltpu.roll(x, shift, axis)


def kernel(cores, count, tile, height, wind_u, wind_v, sqrt_g, metric_aa, metric_ab, metric_bb, coriolis,
           topography, coef_e, coef_c, tracers, out_h, out_u, out_v, out_q,
           dyn_a, dyn_b, tra_a, tra_b, stat, area, aux, coef, pack, ghost_t, ghost_d, ghost_q,
           *traffic):
    slots = 6 // cores
    fields = tracers.shape[0]
    plan = Plan(lax.axis_index('panel'), lax.axis_index('tx'), lax.axis_index('ty'), cores, count)
    edges = [[plan.edge(s, e) for e in range(EDGES)] for s in range(slots)]
    corners = [[plan.corner(s, k // 2, k % 2) for k in range(EDGES)] for s in range(slots)]
    lone = [plan.lone(k // 2, k % 2) for k in range(EDGES)]
    stays = [[plan.here(edges[s][e]) if plan.can_stay(s, e) else None for e in range(EDGES)] for s in range(slots)]
    lanes = lambda rows: lax.broadcasted_iota(jnp.int32, (rows, LANES), 1)
    lane = lanes(1)
    lane8 = lax.broadcasted_iota(jnp.int32, (8, LANES), 1)
    even8 = lax.broadcasted_iota(jnp.int32, (8, LANES), 0) % 2 == 0
    last_lane = tile - LANES - 1
    inner = pl.ds(TOP, tile)
    one = lambda k: pl.ds(k, 1)

    def where_to(found):
        return {'panel': found[0], 'tx': found[1], 'ty': found[2]}

    of_dyn, of_tra, of_end = (traffic[k::BASE] for k in range(BASE))

    def start(kind, par, index, found, stay=None):
        send, recv, spare, sent, landed = kind

        def away():
            pltpu.make_async_remote_copy(
                src_ref=send.at[par, index], dst_ref=recv.at[par, found[-1]], send_sem=sent.at[par],
                recv_sem=landed.at[par], device_id=where_to(found), device_id_type=pl.DeviceIdType.MESH).start()

        def inside():
            pltpu.make_async_copy(send.at[par, index], recv.at[par, found[-1]], landed.at[par]).start()
            pltpu.make_async_copy(send.at[par, index], spare.at[par, index], sent.at[par]).start()
        if stay is None:
            away()
        else:
            pl.when(stay == 0)(away)
            pl.when(stay == 1)(inside)

    def wait_for(kind, par):
        send, recv, _, sent, landed = kind
        pltpu.make_async_copy(recv.at[par], recv.at[par], landed.at[par]).wait()
        pltpu.make_async_copy(send.at[par], send.at[par], sent.at[par]).wait()

    of_end[1][...] = jnp.zeros_like(of_end[1])
    barrier = pltpu.get_barrier_semaphore()
    expected = 0
    for s in range(slots):
        for e in range(EDGES):
            stay = 0 if stays[s][e] is None else stays[s][e]

            def tell(s=s, e=e):
                pl.semaphore_signal(barrier, inc=1, device_id=where_to(edges[s][e]), device_id_type=pl.DeviceIdType.MESH)
            if stays[s][e] is None:
                tell()
            else:
                pl.when(stay == 0)(tell)
            expected = expected + 1 - stay
        for k in range(EDGES):
            @pl.when(lone[k] == 0)
            def _(s=s, k=k):
                pl.semaphore_signal(barrier, inc=1, device_id=where_to(corners[s][k]), device_id_type=pl.DeviceIdType.MESH)
            expected = expected + 1 - lone[k]

    def swap_pairs(x):
        return jnp.where(even8, roll(x, -1, 0), roll(x, 1, 0))

    def send_all(kind, par):
        for s in range(slots):
            for e in range(EDGES):
                start(kind, par, EDGES * s + e, edges[s][e], stays[s][e])

    def pack_columns(src, count_f, depth, send, par):
        def step(i, carry):
            r0 = pl.multiple_of(ROWSP * i, ROWSP)
            rows = pl.ds(r0 + TOP, ROWSP)
            lane = lanes(ROWSP)
            packed = jnp.zeros((ROWSP, LANES), F32)
            for s in range(slots):
                for f in range(count_f):
                    low = TOP * s + depth * f
                    high = low + tile - LANES - depth
                    x = roll(jnp.where(lane < TOP, src(s)[f, 0, rows, :], src(s)[f, 1, rows, :]), low, 1)
                    own = (lane >= low) & (lane < low + depth) | (lane >= high) & (lane < high + depth)
                    packed = jnp.where(own, x, packed)
            packed = jnp.where(lane < SPLIT, packed, roll(packed, depth, 1))
            pack[pl.ds(r0, ROWSP), :] = packed
            return carry
        lax.fori_loop(0, tile // ROWSP, step, 0)
        turned0 = jnp.transpose(pack[:LANES])
        turned1 = jnp.transpose(pack[LANES:])
        for s in range(slots):
            for side in range(DEPTH):
                g = TOP * s + (tile - LANES) * side
                left = turned0[g:g + TOP]
                right = jnp.where(lane8 < tile - LANES, turned1[g:g + TOP], left)
                if side and depth == DEPTH:
                    left, right = swap_pairs(left), swap_pairs(right)
                index = EDGES * s + DEPTH + side
                send[par, index, 0] = left
                send[par, index, 1] = right

    def pack_rows(src, count_f, depth, send, par):
        for s in range(slots):
            for f in range(count_f):
                for d in range(depth):
                    k = one(depth * f + d)
                    send[par, EDGES * s, :, k, :] = src(s)[f, :, one(TOP + d), :]
                    send[par, EDGES * s + 1, :, k, :] = src(s)[f, :, one(tile + TOP - 1 - d), :]

    def send_corners(src, par):
        send = of_end[0]
        for s in range(slots):
            for k in range(EDGES):
                end_a, end_b = divmod(k, DEPTH)
                row = tile + TOP - 1 if end_a else TOP
                at = last_lane if end_b else 0
                for f in range(1, BASE):
                    cell = src(s)[f, end_b, one(row), one(at)]
                    send[par, EDGES * s + k, one(f - 1), :] = jnp.broadcast_to(cell, (1, LANES))
        for s in range(slots):
            for k in range(EDGES):
                found = corners[s][k]
                mine = EDGES * s + k
                start(of_end, par, mine, found[:-1] + (mix(lone[k], mine, found[-1]),), lone[k])

    def unpack(dst, count_f, depth, kind, par, ghosts, lean, turn):
        recv = kind[1]
        wait_for(kind, par)
        ends = {}
        for s in range(slots):
            for e in range(EDGES):
                index = EDGES * s + e
                left, right = recv[par, index, 0], recv[par, index, 1]
                flip = plan.flip(s, e)
                if flip is not None:
                    flipped = (jnp.zeros_like(lane8) + flip) == 1
                    mirror = lane8 ^ last_lane
                    back = jnp.take_along_axis(right, mirror, axis=1)
                    forth = jnp.take_along_axis(left, mirror, axis=1)
                    left, right = jnp.where(flipped, back, left), jnp.where(flipped, forth, right)
                if turn:
                    both = []
                    for lr, x in enumerate((left, right)):
                        stay, down, up = (coef_e[index, lr, k] for k in range(BASE))
                        both.append(stay * x + down * roll(x, DEPTH, 0) + up * roll(x, -DEPTH, 0))
                    left, right = both
                if e < DEPTH:
                    for f in range(count_f):
                        for d in range(depth):
                            k = depth * f + d
                            row = one(tile + TOP + d if e else TOP - 1 - d)
                            dst(s)[f, 0, row, :] = left[k:k + 1]
                            dst(s)[f, 1, row, :] = right[k:k + 1]
                    ends[s, e] = (left, right)
                else:
                    if e == DEPTH and depth == DEPTH:
                        left, right = swap_pairs(left), swap_pairs(right)
                    g = pl.ds(TOP * s + (tile - LANES) * (e - DEPTH), TOP)
                    ghost_t[0, g, :] = jnp.where(lane8 < HALF, left, right)
                    ghost_t[1, g, :] = right
        low = jnp.transpose(ghost_t[0])
        high = jnp.transpose(ghost_t[1])[:tile - LANES]
        low = jnp.where(lanes(LANES) < SPLIT, low, roll(low, lean, 1))
        high = jnp.where(lanes(tile - LANES) < SPLIT, high, roll(high, lean, 1))
        for s in range(slots):
            shift = -TOP * s
            ghosts[s, pl.ds(TOP, LANES), :] = roll(low, shift, 1)
            ghosts[s, pl.ds(TOP + LANES, tile - LANES), :] = roll(high, shift, 1)
        return ends

    def unpack_corners(par, ends):
        wait_for(of_end, par)
        for s in range(slots):
            rows = [jnp.zeros((1, LANES), F32)] * DEPTH
            for k in range(EDGES):
                end_a, end_b = divmod(k, DEPTH)
                x = of_end[1][par, EDGES * s + k]
                stay, down, up = (coef_c[EDGES * s + k, j] for j in range(BASE))
                x = stay * x + down * roll(x, 1, 0) + up * roll(x, -1, 0)
                alone = (jnp.zeros_like(lane) + lone[k]) == 1
                edge_row = ends[s, end_a][end_b]
                at = last_lane if end_b else 0
                for f in range(1, BASE):
                    mirrored = jnp.broadcast_to(edge_row[DEPTH * f:DEPTH * f + 1, at:at + 1], (1, LANES))
                    value = jnp.where(alone, mirrored, x[f - 1:f])
                    place = DEPTH * f + (tile - LANES + DEPTH if end_b else 1)
                    rows[end_a] = jnp.where(lane == place, value, rows[end_a])
            ghost_d[s, one(TOP - 1), :] = rows[0]
            ghost_d[s, one(tile + TOP), :] = rows[1]

    def with_columns(x, ghosts, low):
        lane = lanes(x.shape[1])
        ghosts = roll(ghosts, -DEPTH - low, 1)
        left = jnp.where(lane >= LANES - DEPTH, ghosts, x[0])
        right = jnp.where((lane == tile - LANES) | (lane == tile - LANES + 1), ghosts, x[1])
        return jnp.stack([left, right])

    def refresh(state, count_f):
        def step(f, carry):
            for s in range(slots):
                left, right = state(s)[f, 0, inner, :], state(s)[f, 1, inner, :]
                lane = lanes(tile)
                state(s)[f, 0, inner, :] = jnp.where(lane < HALF, left, right)
                state(s)[f, 1, inner, :] = jnp.where((lane < HALF) & (lane >= tile - LANES), left, right)
            return carry
        lax.fori_loop(0, count_f, step, 0)

    def take(src, dst):
        dst[0, inner, :] = src[:, :LANES]
        dst[1, inner, :] = src[:, :LANES]
        dst[1, inner, :tile - LANES] = src[:, LANES:]

    zero_rows = jnp.zeros((2 * LANES - tile, LANES), F32)
    pack[tile:2 * LANES, :] = zero_rows
    ghost_t[...] = jnp.zeros_like(ghost_t)
    ghost_d[...] = jnp.zeros_like(ghost_d)
    ghost_q[...] = jnp.zeros_like(ghost_q)
    for kind in (of_dyn, of_end):
        kind[0][...] = jnp.zeros_like(kind[0])
    group0 = lambda s: stat.at[s, 0]
    group1 = lambda s: stat.at[s, 1]
    def take_state(s, carry):
        for k, ref in enumerate((sqrt_g, metric_aa, metric_ab)):
            take(ref.at[s], stat.at[s, 0, k])
        for k, ref in enumerate((metric_bb, topography, coriolis)):
            take(ref.at[s], stat.at[s, 1, k])
        for k, ref in enumerate((height, wind_u, wind_v)):
            take(ref.at[s], dyn_a.at[s, k])
        return carry
    lax.fori_loop(0, slots, take_state, 0)
    dyn_of = {0: lambda s: dyn_a.at[s], 1: lambda s: dyn_b.at[s]}
    tra_of = {0: lambda s: tra_a.at[s], 1: lambda s: tra_b.at[s]}
    groups = (DEPTH, group0), (BASE, group1)
    for par, group in groups:
        pack_columns(group, BASE, DEPTH, of_dyn[0], par)
        pack_rows(group, BASE, DEPTH, of_dyn[0], par)
        if par == DEPTH:
            pl.semaphore_wait(barrier, expected)
        send_all(of_dyn, par)

    def pack_dyn(par):
        pack_columns(dyn_of[par], BASE, DEPTH, of_dyn[0], par)
        pack_rows(dyn_of[par], BASE, DEPTH, of_dyn[0], par)
        send_all(of_dyn, par)
        send_corners(dyn_of[par], par)

    def pack_tra(par):
        pack_columns(tra_of[par], fields, 1, of_tra[0], par)
        pack_rows(tra_of[par], fields, 1, of_tra[0], par)
        send_all(of_tra, par)

    pack_dyn(0)
    def take_tracer(t, carry):
        for s in range(slots):
            take(tracers.at[t, s], tra_a.at[s, t])
        return carry
    lax.fori_loop(0, fields, take_tracer, 0)
    pack_tra(0)

    for par, group in groups:
        unpack(group, BASE, DEPTH, of_dyn, par, ghost_d, DEPTH, False)
        def fill_slot(s, carry):
            def fill(i, carry):
                rows = pl.ds(pl.multiple_of(ROWSP * i, ROWSP) + 8, ROWSP)
                g = ghost_d[s, rows, :]
                for f in range(3):
                    group(s)[f, :, rows, :] = with_columns(group(s)[f, :, rows, :], g, 2 * f)
                if par == DEPTH:
                    inverse = 1.0 / group(s)[0, :, rows, :]
                    area[s, 0, :, rows, :] = inverse
                    area[s, 1, :, rows, :] = (-0.5 * TIME_STEP) * inverse
                return carry
            return lax.fori_loop(0, tile // ROWSP, fill, carry)
        lax.fori_loop(0, slots, fill_slot, 0)

    def by_blocks(part, total, count_r, count_p):
        def step(i, carry):
            for k in range(count_p):
                part(pl.multiple_of(count_r * count_p * i, TOP) + count_r * k)
            return carry
        lax.fori_loop(0, total // (count_r * count_p), step, 0)

    def first_pass(s, now):
        state = dyn_of[now](s)

        def part(r0):
            rows = pl.ds(r0, ROWS1)
            g = ghost_d[s, rows, :]
            h, u, v = (with_columns(state[f, :, rows, :], g, 2 * f) for f in range(3))
            state[0, :, rows, :] = h
            state[1, :, rows, :] = u
            state[2, :, rows, :] = v
            jac, gaa, gab = (stat[s, 0, k, :, rows, :] for k in range(3))
            gbb, top = (stat[s, 1, k, :, rows, :] for k in range(2))
            contra_a = gaa * u + gab * v
            contra_b = gab * u + gbb * v
            jh = jac * h
            aux[0, :, rows, :] = GRAVITY * (h + top) + 0.5 * (u * contra_a + v * contra_b)
            aux[1, :, rows, :] = jh * contra_a
            aux[2, :, rows, :] = jh * contra_b
            aux[3, :, rows, :] = contra_a
            aux[4, :, rows, :] = contra_b
        by_blocks(part, tile + DEPTH * TOP, ROWS1, PARTS1)

    def second_pass(s, now):
        state, fresh = dyn_of[now](s), dyn_of[1 - now](s)

        def part(r0):
            r0 = r0 + TOP

            def at(ref, f, shift=0):
                return ref[f, :, pl.ds(r0 + shift, ROWS2), :]
            rows = pl.ds(r0, ROWS2)
            h, u, v = (at(state, f) for f in range(3))
            area_here = area.at[s]
            inv_jac = at(area_here, 0)
            jac = at(stat.at[s, 0], 0)
            mass_a = at(aux, 1)
            plus, minus = mass_a + h, mass_a - h
            flux_e = plus + (at(aux, 1, 1) - at(state, 0, 1))
            flux_w = (at(aux, 1, -1) + at(state, 0, -1)) + minus
            mass_b = at(aux, 2)
            plus_b, minus_b = mass_b + h, mass_b - h
            flux_n = plus_b + roll(minus_b, -1, 2)
            flux_s = roll(plus_b, 1, 2) + minus_b
            total = (flux_e - flux_w) + (flux_n - flux_s)
            h_t = (-0.5) * total * inv_jac
            coef[s, 0, :, rows, :] = 0.5 * total + 4.0
            coef[s, 1, :, rows, :] = 0.5 * flux_e - 1.0
            coef[s, 2, :, rows, :] = -0.5 * flux_w - 1.0
            coef[s, 3, :, rows, :] = 0.5 * flux_n - 1.0
            coef[s, 4, :, rows, :] = -0.5 * flux_s - 1.0
            twelfth = 1.0 / 12.0
            e = at(aux, 0)
            slope_a = (8.0 * (at(aux, 0, 1) - at(aux, 0, -1)) - (at(aux, 0, 2) - at(aux, 0, -2))) * twelfth
            slope_b = (8.0 * (roll(e, -1, 2) - roll(e, 1, 2)) - (roll(e, -2, 2) - roll(e, 2, 2))) * twelfth
            v_e, v_w = at(state, 2, 1), at(state, 2, -1)
            turn_v = (8.0 * (v_e - v_w) - (at(state, 2, 2) - at(state, 2, -2))) * twelfth
            u_n, u_s = roll(u, -1, 2), roll(u, 1, 2)
            turn_u = (8.0 * (u_n - u_s) - (roll(u, -2, 2) - roll(u, 2, 2))) * twelfth
            spin = ((turn_v - turn_u) * inv_jac + at(stat.at[s, 1], 2)) * jac
            pair_u = at(state, 1, 1) + at(state, 1, -1)
            lap_u = (4.0 * (pair_u + (u_n + u_s)) + (roll(pair_u, -1, 2) + roll(pair_u, 1, 2)) - 20.0 * u) * (1.0 / 6.0)
            pair_v = v_e + v_w
            mid_v = 4.0 * v + pair_v
            lap_v = (4.0 * pair_v + (roll(mid_v, -1, 2) + roll(mid_v, 1, 2)) - 20.0 * v) * (1.0 / 6.0)
            u_t = spin * at(aux, 4) - slope_a + WAVE_SPEED * lap_u
            v_t = WAVE_SPEED * lap_v - spin * at(aux, 3) - slope_b
            for f, (x, x_t) in enumerate(((h, h_t), (u, u_t), (v, v_t))):
                new = x + TIME_STEP * x_t
                if now == 1:
                    new = 0.5 * (at(fresh, f) + new)
                fresh[f, :, rows, :] = new
        by_blocks(part, tile, ROWS2, PARTS2)

    def tracer_pass(s, now):
        state, fresh = tra_of[now](s), tra_of[1 - now](s)

        def part(r0):
            r0 = r0 + TOP
            rows = pl.ds(r0, ROWSB)
            g = ghost_q[s, rows, :]
            mid, east, west, north, south = (coef[s, k, :, rows, :] for k in range(5))
            scale = area[s, 1, :, rows, :]
            lane = lanes(ROWSB)
            for t in range(fields):
                q = state[t, :, rows, :]
                q_e = state[t, :, pl.ds(r0 + 1, ROWSB), :]
                q_w = state[t, :, pl.ds(r0 - 1, ROWSB), :]
                ghost = roll(g, -t, 1)
                q_n, q_s = roll(q, -1, 2), roll(q, 1, 2)
                q_s = jnp.stack([jnp.where(lane == 0, ghost, q_s[0]), q_s[1]])
                q_n = jnp.stack([q_n[0], jnp.where(lane == last_lane, ghost, q_n[1])])
                total = mid * q + (east * q_e + west * q_w) + (north * q_n + south * q_s)
                new = q + scale * total
                if now == 1:
                    new = 0.5 * (fresh[t, :, rows, :] + new)
                fresh[t, :, rows, :] = new
        by_blocks(part, tile, ROWSB, PARTSB)

    def stage(now, more):
        ends = unpack(dyn_of[now], BASE, DEPTH, of_dyn, now, ghost_d, DEPTH, True)
        unpack_corners(now, ends)

        def cells(s, carry):
            first_pass(s, now)
            second_pass(s, now)
            return carry
        lax.fori_loop(0, slots, cells, 0)

        def forward(send):
            if more is None:
                send(1 - now)
            else:
                pl.when(more)(lambda: send(1 - now))
        forward(pack_dyn)
        unpack(tra_of[now], fields, 1, of_tra, now, ghost_q, -1, False)

        def tracers_of(s, carry):
            tracer_pass(s, now)
            return carry
        lax.fori_loop(0, slots, tracers_of, 0)
        forward(pack_tra)

    def one_step(step_index, carry):
        @pl.when(step_index == STEPS // DEPTH)
        def _():
            refresh(dyn_of[0], BASE)
            refresh(tra_of[0], fields)
        stage(0, None)
        stage(1, step_index < STEPS - 1)
        return carry

    lax.fori_loop(0, STEPS, one_step, 0)

    def give(src, dst):
        x0, x1 = src[0, inner, :], src[1, inner, :]
        dst[:, :LANES] = jnp.where(lanes(tile) < HALF, x0, x1)
        dst[:, LANES:] = x1[:, :tile - LANES]

    def give_tracer(t, carry):
        for s in range(slots):
            give(tra_a.at[s, t], out_q.at[t, s])
        return carry
    lax.fori_loop(0, fields, give_tracer, 0)

    def give_state(s, carry):
        for k, ref in enumerate((out_h, out_u, out_v)):
            give(dyn_a.at[s, k], ref.at[s])
        return carry
    lax.fori_loop(0, slots, give_state, 0)


def coefficients(rotation, pos_a, pos_b, count, tile):
    slots = rotation.shape[0]
    line = jnp.transpose(rotation, (0, 1, 3, 4, 2)).reshape(slots, 4, 4, rotation.shape[2])
    line = jnp.pad(line, ((0, 0), (0, 0), (0, 0), (2, LANES)))
    along = lambda part, pos: lax.dynamic_slice_in_dim(part, pos * tile, 2 * LANES, axis=3)
    line = jnp.concatenate([along(line[:, 0:2], pos_b), along(line[:, 2:4], pos_a)], axis=1)
    edge = jnp.stack([pos_a == 0, pos_a == count - 1, pos_b == 0, pos_b == count - 1])
    one = jnp.array([1.0, 0.0, 0.0, 1.0], F32)[:, None]
    line = jnp.where(edge[:, None, None], line, one)
    left = jnp.concatenate([line[..., 2:LANES], line[..., 0:2]], axis=-1)
    right = jnp.concatenate([line[..., LANES + 2:LANES + 2 + TOP * TOP + DEPTH], line[..., TOP * TOP + DEPTH + 2:LANES + 2]], axis=-1)
    m = jnp.stack([left, right], axis=2)
    m = m.reshape(slots * 4, 2, 4, LANES)
    zero = jnp.zeros_like(m[:, :, 0])
    unit = jnp.ones_like(zero)
    m00, m01, m10, m11 = (m[:, :, k] for k in range(EDGES))
    stay = jnp.stack([unit, unit, m00, m00, m11, m11, zero, zero], axis=2)
    down = jnp.stack([zero, zero, zero, zero, m10, m10, zero, zero], axis=2)
    up = jnp.stack([zero, zero, m01, m01, zero, zero, zero, zero], axis=2)
    coef_e = jnp.stack([stay, down, up], axis=2)

    before, after = line[..., 1], line[..., tile + 2]
    found = []
    for k in range(EDGES):
        end_a, end_b = k // 2, k % 2
        by_a = (after if end_b else before)[:, end_a]
        by_b = (after if end_a else before)[:, 2 + end_b]
        found.append(jnp.where(edge[end_a], by_a, by_b))
    c = jnp.stack(found, axis=1).reshape(slots * 4, 4)
    zero = jnp.zeros_like(c[:, 0])
    rows = jnp.stack([jnp.stack([c[:, 0], c[:, 3]], -1), jnp.stack([zero, c[:, 2]], -1), jnp.stack([c[:, 1], zero], -1)], axis=1)
    rows = jnp.pad(rows, ((0, 0), (0, 0), (0, 6)))
    return coef_e, jnp.broadcast_to(rows[..., None], rows.shape + (LANES,))


def solution(mesh):
    cores, count = mesh.shape['panel'], mesh.shape['tx']
    slots = 6 // cores

    def body(height, wind_u, wind_v, sqrt_g, metric_aa, metric_ab, metric_bb, coriolis, topography, rotation, tracers):
        tile = height.shape[-1]
        fields = tracers.shape[0]
        coef_e, coef_c = coefficients(rotation, lax.axis_index('tx'), lax.axis_index('ty'), count, tile)
        rows = tile + DEPTH * TOP
        vmem = lambda *shape: pltpu.VMEM(shape, F32)
        blocks = (DEPTH, rows, LANES)
        state = [vmem(slots, count_f, *blocks) for count_f in (BASE, BASE, fields, fields)]
        messages = slots * EDGES
        buffers = [vmem(DEPTH + DEPTH, messages, DEPTH, TOP, LANES), vmem(DEPTH, messages, DEPTH, TOP, LANES),
                   vmem(DEPTH, messages, TOP, LANES)]
        counters = [pltpu.SemaphoreType.DMA((count_p,)) for count_p in (DEPTH + DEPTH, DEPTH, DEPTH)]
        whole = pl.BlockSpec(memory_space=pltpu.VMEM)
        args = (height, wind_u, wind_v, sqrt_g, metric_aa, metric_ab, metric_bb, coriolis, topography, coef_e, coef_c, tracers)
        outs = [jax.ShapeDtypeStruct(x.shape, F32) for x in (height, wind_u, wind_v, tracers)]
        call = pl.pallas_call(
            functools.partial(kernel, cores, count, tile),
            out_shape=outs,
            in_specs=[whole] * len(args),
            out_specs=[whole] * len(outs),
            scratch_shapes=state + [
                vmem(slots, DEPTH, BASE, *blocks), vmem(slots, DEPTH, *blocks),
                vmem(BASE + DEPTH, *blocks), vmem(slots, BASE + DEPTH, *blocks),
                vmem(DEPTH * LANES, LANES), vmem(DEPTH, LANES, LANES), vmem(slots, rows, LANES), vmem(slots, rows, LANES),
            ] + buffers * BASE + counters * DEPTH,
            compiler_params=pltpu.CompilerParams(
                collective_id=0, has_side_effects=True, vmem_limit_bytes=63 << 20),
            name='swe',
        )
        return tuple(call(*args))

    state_spec = P(('member', 'panel'), 'tx', 'ty')
    static_spec = P('panel', 'tx', 'ty')
    tracer_spec = P(None, ('member', 'panel'), 'tx', 'ty')
    in_specs = (state_spec, state_spec, state_spec, static_spec, static_spec, static_spec, static_spec, static_spec, static_spec, P('panel'), tracer_spec)
    out_specs = (state_spec, state_spec, state_spec, tracer_spec)
    return jax.shard_map(body, mesh=mesh, in_specs=in_specs, out_specs=out_specs, check_vma=False)
```

```python
import functools

import jax
import jax.numpy as jnp
from jax import lax
from jax.experimental import pallas as pl
from jax.experimental.pallas import tpu as pltpu
from jax.sharding import PartitionSpec as P

STEPS = 8
TIME_STEP = 0.1
GRAVITY = 1.0
WAVE_SPEED = 1.0
LINKS = (
    '310 100 530 420',
    '010 200 511 410',
    '110 300 521 431',
    '210 000 500 401',
    '331 130 030 231',
    '320 121 221 020',
)
NEIGHBOURS = tuple(tuple(tuple(map(int, link)) for link in row.split()) for row in LINKS)
LANES = 128
HALF = 96
TOP = 8
EDGES = 4
BASE = 3
DEPTH = 2
SPLIT = 32
ROWS1, PARTS1 = 104, 1
ROWS2, PARTS2 = 48, 1
ROWSB, PARTSB = 16, 4
ROWSP = 96
F32 = jnp.float32


def pick(index, values):
    if all(value is values[0] for value in values):
        return values[0]
    total = 0
    for place, value in enumerate(values):
        total = total + same(index, place) * value
    return total


def same(x, y):
    return 1 - lax.min((x - y) * (x - y), 1)


def mix(cond, yes, no):
    return cond * yes + (1 - cond) * no


def on_edge(edge, along, count):
    if edge == 0:
        return 0, along
    if edge == 1:
        return count - 1, along
    if edge == 2:
        return along, 0
    return along, count - 1


class Plan:
    def __init__(self, core, pos_a, pos_b, cores, count):
        self.core, self.pos_a, self.pos_b = core, pos_a, pos_b
        self.cores, self.count = cores, count
        self.slots = 6 // cores
        first = lambda x: 1 - lax.div(x + count - 1, count)
        last = lambda x: lax.div(x + 1, count)
        self.at_edge = (first(pos_a), last(pos_a), first(pos_b), last(pos_b))

    def across(self, slot, edge, along, side=None):
        found = []
        for core in range(self.cores):
            other, other_edge, flipped = NEIGHBOURS[core * self.slots + slot][edge]
            place = self.count - 1 - along if flipped else along
            tile_a, tile_b = on_edge(other_edge, place, self.count)
            if side is None:
                index = (other % self.slots) * EDGES + other_edge
            else:
                end = 1 - side if flipped else side
                if other_edge < 2:
                    index = (other % self.slots) * EDGES + 2 * other_edge + end
                else:
                    index = (other % self.slots) * EDGES + 2 * end + other_edge - 2
            found.append((other // self.slots, tile_a, tile_b, index))
        return tuple(pick(self.core, [entry[k] for entry in found]) for k in range(EDGES))

    def edge(self, slot, edge):
        along = self.pos_b if edge < 2 else self.pos_a
        out = self.across(slot, edge, along)
        step = 1 if edge % 2 else -1
        inside = (
            self.core,
            self.pos_a + (step if edge < 2 else 0),
            self.pos_b + (0 if edge < 2 else step),
            slot * EDGES + (edge ^ 1),
        )
        return tuple(mix(self.at_edge[edge], o, i) for o, i in zip(out, inside))

    def corner(self, slot, end_a, end_b):
        step_a, step_b = 2 * end_a - 1, 2 * end_b - 1
        out_a, out_b = self.at_edge[end_a], self.at_edge[2 + end_b]
        by_a = self.across(slot, end_a, self.pos_b + step_b, 1 - end_b)
        by_b = self.across(slot, 2 + end_b, self.pos_a + step_a, 1 - end_a)
        inside = (self.core, self.pos_a + step_a, self.pos_b + step_b, slot * EDGES + 2 * (1 - end_a) + 1 - end_b)
        return tuple(mix(out_a, x, mix(out_b, y, z)) for x, y, z in zip(by_a, by_b, inside))

    def lone(self, end_a, end_b):
        return self.at_edge[end_a] * self.at_edge[2 + end_b]

    def here(self, found):
        return same(found[0], self.core) * same(found[1], self.pos_a) * same(found[2], self.pos_b)

    def can_stay(self, slot, edge):
        for core in range(self.cores):
            other, other_edge, flipped = NEIGHBOURS[core * self.slots + slot][edge]
            if other // self.slots == core:
                for along in range(self.count):
                    place = self.count - 1 - along if flipped else along
                    if on_edge(edge, along, self.count) == on_edge(other_edge, place, self.count):
                        return True
        return False

    def flip(self, slot, edge):
        values = [NEIGHBOURS[core * self.slots + slot][edge][2] for core in range(self.cores)]
        if not any(values):
            return None
        return self.at_edge[edge] * pick(self.core, values)


def roll(x, shift, axis):
    shift = shift % x.shape[axis]
    return x if shift == 0 else pltpu.roll(x, shift, axis)


def kernel(cores, count, tile, height, wind_u, wind_v, sqrt_g, metric_aa, metric_ab, metric_bb, coriolis,
           topography, coef_e, coef_c, tracers, dyn_a, tra_a,
           dyn_b, tra_b, stat, area, aux, coef, pack, ghost_t, ghost_d, ghost_q,
           *traffic):
    slots = 6 // cores
    fields = tracers.shape[0]
    plan = Plan(lax.axis_index('panel'), lax.axis_index('tx'), lax.axis_index('ty'), cores, count)
    edges = [[plan.edge(s, e) for e in range(EDGES)] for s in range(slots)]
    corners = [[plan.corner(s, k // 2, k % 2) for k in range(EDGES)] for s in range(slots)]
    lone = [plan.lone(k // 2, k % 2) for k in range(EDGES)]
    stays = [[plan.here(edges[s][e]) if plan.can_stay(s, e) else None for e in range(EDGES)] for s in range(slots)]
    lanes = lambda rows: lax.broadcasted_iota(jnp.int32, (rows, LANES), 1)
    lane = lanes(1)
    lane8 = lax.broadcasted_iota(jnp.int32, (8, LANES), 1)
    even8 = lax.broadcasted_iota(jnp.int32, (8, LANES), 0) % 2 == 0
    last_lane = tile - LANES - 1
    inner = pl.ds(TOP, tile)
    one = lambda k: pl.ds(k, 1)

    def where_to(found):
        return {'panel': found[0], 'tx': found[1], 'ty': found[2]}

    of_dyn, of_tra, of_end = (traffic[k::BASE] for k in range(BASE))

    def start(kind, par, index, found, stay=None):
        send, recv, spare, sent, landed = kind

        def away():
            pltpu.make_async_remote_copy(
                src_ref=send.at[par, index], dst_ref=recv.at[par, found[-1]], send_sem=sent.at[par],
                recv_sem=landed.at[par], device_id=where_to(found), device_id_type=pl.DeviceIdType.MESH).start()

        def inside():
            pltpu.make_async_copy(send.at[par, index], recv.at[par, found[-1]], landed.at[par]).start()
            pltpu.make_async_copy(send.at[par, index], spare.at[par, index], sent.at[par]).start()
        if stay is None:
            away()
        else:
            pl.when(stay == 0)(away)
            pl.when(stay == 1)(inside)

    def wait_for(kind, par):
        send, recv, _, sent, landed = kind
        pltpu.make_async_copy(recv.at[par], recv.at[par], landed.at[par]).wait()
        pltpu.make_async_copy(send.at[par], send.at[par], sent.at[par]).wait()

    of_end[1][...] = jnp.zeros_like(of_end[1])
    barrier = pltpu.get_barrier_semaphore()
    expected = 0
    for s in range(slots):
        for e in range(EDGES):
            stay = 0 if stays[s][e] is None else stays[s][e]

            def tell(s=s, e=e):
                pl.semaphore_signal(barrier, inc=1, device_id=where_to(edges[s][e]), device_id_type=pl.DeviceIdType.MESH)
            if stays[s][e] is None:
                tell()
            else:
                pl.when(stay == 0)(tell)
            expected = expected + 1 - stay
        for k in range(EDGES):
            @pl.when(lone[k] == 0)
            def _(s=s, k=k):
                pl.semaphore_signal(barrier, inc=1, device_id=where_to(corners[s][k]), device_id_type=pl.DeviceIdType.MESH)
            expected = expected + 1 - lone[k]

    def swap_pairs(x):
        return jnp.where(even8, roll(x, -1, 0), roll(x, 1, 0))

    def send_all(kind, par):
        for s in range(slots):
            for e in range(EDGES):
                start(kind, par, EDGES * s + e, edges[s][e], stays[s][e])

    def pack_columns(src, count_f, depth, send, par):
        def step(i, carry):
            r0 = pl.multiple_of(ROWSP * i, ROWSP)
            rows = pl.ds(r0 + TOP, ROWSP)
            lane = lanes(ROWSP)
            packed = jnp.zeros((ROWSP, LANES), F32)
            for s in range(slots):
                for f in range(count_f):
                    low = TOP * s + depth * f
                    high = low + tile - LANES - depth
                    x = roll(jnp.where(lane < TOP, src(s)[f, 0, rows, :], src(s)[f, 1, rows, :]), low, 1)
                    own = (lane >= low) & (lane < low + depth) | (lane >= high) & (lane < high + depth)
                    packed = jnp.where(own, x, packed)
            packed = jnp.where(lane < SPLIT, packed, roll(packed, depth, 1))
            pack[pl.ds(r0, ROWSP), :] = packed
            return carry
        lax.fori_loop(0, tile // ROWSP, step, 0)
        turned0 = jnp.transpose(pack[:LANES])
        turned1 = jnp.transpose(pack[LANES:])
        for s in range(slots):
            for side in range(DEPTH):
                g = TOP * s + (tile - LANES) * side
                left = turned0[g:g + TOP]
                right = jnp.where(lane8 < tile - LANES, turned1[g:g + TOP], left)
                if side and depth == DEPTH:
                    left, right = swap_pairs(left), swap_pairs(right)
                index = EDGES * s + DEPTH + side
                send[par, index, 0] = left
                send[par, index, 1] = right

    def pack_rows(src, count_f, depth, send, par):
        for s in range(slots):
            for f in range(count_f):
                for d in range(depth):
                    k = one(depth * f + d)
                    send[par, EDGES * s, :, k, :] = src(s)[f, :, one(TOP + d), :]
                    send[par, EDGES * s + 1, :, k, :] = src(s)[f, :, one(tile + TOP - 1 - d), :]

    def send_corners(src, par):
        send = of_end[0]
        for s in range(slots):
            for k in range(EDGES):
                end_a, end_b = divmod(k, DEPTH)
                row = tile + TOP - 1 if end_a else TOP
                at = last_lane if end_b else 0
                for f in range(1, BASE):
                    cell = src(s)[f, end_b, one(row), one(at)]
                    send[par, EDGES * s + k, one(f - 1), :] = jnp.broadcast_to(cell, (1, LANES))
        for s in range(slots):
            for k in range(EDGES):
                found = corners[s][k]
                mine = EDGES * s + k
                start(of_end, par, mine, found[:-1] + (mix(lone[k], mine, found[-1]),), lone[k])

    def unpack(dst, count_f, depth, kind, par, ghosts, lean, turn):
        recv = kind[1]
        wait_for(kind, par)
        ends = {}
        for s in range(slots):
            for e in range(EDGES):
                index = EDGES * s + e
                left, right = recv[par, index, 0], recv[par, index, 1]
                flip = plan.flip(s, e)
                if flip is not None:
                    flipped = (jnp.zeros_like(lane8) + flip) == 1
                    mirror = lane8 ^ last_lane
                    back = jnp.take_along_axis(right, mirror, axis=1)
                    forth = jnp.take_along_axis(left, mirror, axis=1)
                    left, right = jnp.where(flipped, back, left), jnp.where(flipped, forth, right)
                if turn:
                    both = []
                    for lr, x in enumerate((left, right)):
                        stay, down, up = (coef_e[index, lr, k] for k in range(BASE))
                        both.append(stay * x + down * roll(x, DEPTH, 0) + up * roll(x, -DEPTH, 0))
                    left, right = both
                if e < DEPTH:
                    for f in range(count_f):
                        for d in range(depth):
                            k = depth * f + d
                            row = one(tile + TOP + d if e else TOP - 1 - d)
                            dst(s)[f, 0, row, :] = left[k:k + 1]
                            dst(s)[f, 1, row, :] = right[k:k + 1]
                    ends[s, e] = (left, right)
                else:
                    if e == DEPTH and depth == DEPTH:
                        left, right = swap_pairs(left), swap_pairs(right)
                    g = pl.ds(TOP * s + (tile - LANES) * (e - DEPTH), TOP)
                    ghost_t[0, g, :] = jnp.where(lane8 < HALF, left, right)
                    ghost_t[1, g, :] = right
        low = jnp.transpose(ghost_t[0])
        high = jnp.transpose(ghost_t[1])[:tile - LANES]
        low = jnp.where(lanes(LANES) < SPLIT, low, roll(low, lean, 1))
        high = jnp.where(lanes(tile - LANES) < SPLIT, high, roll(high, lean, 1))
        for s in range(slots):
            shift = -TOP * s
            ghosts[s, pl.ds(TOP, LANES), :] = roll(low, shift, 1)
            ghosts[s, pl.ds(TOP + LANES, tile - LANES), :] = roll(high, shift, 1)
        return ends

    def unpack_corners(par, ends):
        wait_for(of_end, par)
        for s in range(slots):
            rows = [jnp.zeros((1, LANES), F32)] * DEPTH
            for k in range(EDGES):
                end_a, end_b = divmod(k, DEPTH)
                x = of_end[1][par, EDGES * s + k]
                stay, down, up = (coef_c[EDGES * s + k, j] for j in range(BASE))
                x = stay * x + down * roll(x, 1, 0) + up * roll(x, -1, 0)
                alone = (jnp.zeros_like(lane) + lone[k]) == 1
                edge_row = ends[s, end_a][end_b]
                at = last_lane if end_b else 0
                for f in range(1, BASE):
                    mirrored = jnp.broadcast_to(edge_row[DEPTH * f:DEPTH * f + 1, at:at + 1], (1, LANES))
                    value = jnp.where(alone, mirrored, x[f - 1:f])
                    place = DEPTH * f + (tile - LANES + DEPTH if end_b else 1)
                    rows[end_a] = jnp.where(lane == place, value, rows[end_a])
            ghost_d[s, one(TOP - 1), :] = rows[0]
            ghost_d[s, one(tile + TOP), :] = rows[1]

    def with_columns(x, ghosts, low):
        lane = lanes(x.shape[1])
        ghosts = roll(ghosts, -DEPTH - low, 1)
        left = jnp.where(lane >= LANES - DEPTH, ghosts, x[0])
        right = jnp.where((lane == tile - LANES) | (lane == tile - LANES + 1), ghosts, x[1])
        return jnp.stack([left, right])

    def refresh(state, count_f):
        def step(f, carry):
            for s in range(slots):
                left, right = state(s)[f, 0, inner, :], state(s)[f, 1, inner, :]
                lane = lanes(tile)
                state(s)[f, 0, inner, :] = jnp.where(lane < HALF, left, right)
                state(s)[f, 1, inner, :] = jnp.where((lane < HALF) & (lane >= tile - LANES), left, right)
            return carry
        lax.fori_loop(0, count_f, step, 0)

    def take(src, dst):
        dst[0, inner, :] = src[:, :LANES]
        dst[1, inner, :] = src[:, :LANES]
        dst[1, inner, :tile - LANES] = src[:, LANES:]

    zero_rows = jnp.zeros((2 * LANES - tile, LANES), F32)
    pack[tile:2 * LANES, :] = zero_rows
    ghost_t[...] = jnp.zeros_like(ghost_t)
    ghost_d[...] = jnp.zeros_like(ghost_d)
    ghost_q[...] = jnp.zeros_like(ghost_q)
    for kind in (of_dyn, of_end):
        kind[0][...] = jnp.zeros_like(kind[0])
    group0 = lambda s: stat.at[s, 0]
    group1 = lambda s: stat.at[s, 1]
    def take_state(s, carry):
        for k, ref in enumerate((sqrt_g, metric_aa, metric_ab)):
            take(ref.at[s], stat.at[s, 0, k])
        for k, ref in enumerate((metric_bb, topography, coriolis)):
            take(ref.at[s], stat.at[s, 1, k])
        for k, ref in enumerate((height, wind_u, wind_v)):
            take(ref.at[s], dyn_a.at[s, k])
        return carry
    lax.fori_loop(0, slots, take_state, 0)
    dyn_of = {0: lambda s: dyn_a.at[s], 1: lambda s: dyn_b.at[s]}
    tra_of = {0: lambda s: tra_a.at[s], 1: lambda s: tra_b.at[s]}
    groups = (DEPTH, group0), (BASE, group1)
    for par, group in groups:
        pack_columns(group, BASE, DEPTH, of_dyn[0], par)
        pack_rows(group, BASE, DEPTH, of_dyn[0], par)
        if par == DEPTH:
            pl.semaphore_wait(barrier, expected)
        send_all(of_dyn, par)

    def pack_dyn(par):
        pack_columns(dyn_of[par], BASE, DEPTH, of_dyn[0], par)
        pack_rows(dyn_of[par], BASE, DEPTH, of_dyn[0], par)
        send_all(of_dyn, par)
        send_corners(dyn_of[par], par)

    def pack_tra(par):
        pack_columns(tra_of[par], fields, 1, of_tra[0], par)
        pack_rows(tra_of[par], fields, 1, of_tra[0], par)
        send_all(of_tra, par)

    pack_dyn(0)
    def take_tracer(t, carry):
        for s in range(slots):
            take(tracers.at[t, s], tra_a.at[s, t])
        return carry
    lax.fori_loop(0, fields, take_tracer, 0)
    pack_tra(0)

    for par, group in groups:
        unpack(group, BASE, DEPTH, of_dyn, par, ghost_d, DEPTH, False)
        def fill_slot(s, carry):
            def fill(i, carry):
                rows = pl.ds(pl.multiple_of(ROWSP * i, ROWSP) + 8, ROWSP)
                g = ghost_d[s, rows, :]
                for f in range(3):
                    group(s)[f, :, rows, :] = with_columns(group(s)[f, :, rows, :], g, 2 * f)
                if par == DEPTH:
                    inverse = 1.0 / group(s)[0, :, rows, :]
                    area[s, 0, :, rows, :] = inverse
                    area[s, 1, :, rows, :] = (-0.5 * TIME_STEP) * inverse
                return carry
            return lax.fori_loop(0, tile // ROWSP, fill, carry)
        lax.fori_loop(0, slots, fill_slot, 0)

    def by_blocks(part, total, count_r, count_p):
        def step(i, carry):
            for k in range(count_p):
                part(pl.multiple_of(count_r * count_p * i, TOP) + count_r * k)
            return carry
        lax.fori_loop(0, total // (count_r * count_p), step, 0)

    def first_pass(s, now):
        state = dyn_of[now](s)

        def part(r0):
            rows = pl.ds(r0, ROWS1)
            g = ghost_d[s, rows, :]
            h, u, v = (with_columns(state[f, :, rows, :], g, 2 * f) for f in range(3))
            state[0, :, rows, :] = h
            state[1, :, rows, :] = u
            state[2, :, rows, :] = v
            jac, gaa, gab = (stat[s, 0, k, :, rows, :] for k in range(3))
            gbb, top = (stat[s, 1, k, :, rows, :] for k in range(2))
            contra_a = gaa * u + gab * v
            contra_b = gab * u + gbb * v
            jh = jac * h
            aux[0, :, rows, :] = GRAVITY * (h + top) + 0.5 * (u * contra_a + v * contra_b)
            aux[1, :, rows, :] = jh * contra_a
            aux[2, :, rows, :] = jh * contra_b
            aux[3, :, rows, :] = contra_a
            aux[4, :, rows, :] = contra_b
        by_blocks(part, tile + DEPTH * TOP, ROWS1, PARTS1)

    def second_pass(s, now):
        state, fresh = dyn_of[now](s), dyn_of[1 - now](s)

        def part(r0):
            r0 = r0 + TOP

            def at(ref, f, shift=0):
                return ref[f, :, pl.ds(r0 + shift, ROWS2), :]
            rows = pl.ds(r0, ROWS2)
            h, u, v = (at(state, f) for f in range(3))
            area_here = area.at[s]
            inv_jac = at(area_here, 0)
            jac = at(stat.at[s, 0], 0)
            mass_a = at(aux, 1)
            plus, minus = mass_a + h, mass_a - h
            flux_e = plus + (at(aux, 1, 1) - at(state, 0, 1))
            flux_w = (at(aux, 1, -1) + at(state, 0, -1)) + minus
            mass_b = at(aux, 2)
            plus_b, minus_b = mass_b + h, mass_b - h
            flux_n = plus_b + roll(minus_b, -1, 2)
            flux_s = roll(plus_b, 1, 2) + minus_b
            total = (flux_e - flux_w) + (flux_n - flux_s)
            h_t = (-0.5) * total * inv_jac
            coef[s, 0, :, rows, :] = 0.5 * total + 4.0
            coef[s, 1, :, rows, :] = 0.5 * flux_e - 1.0
            coef[s, 2, :, rows, :] = -0.5 * flux_w - 1.0
            coef[s, 3, :, rows, :] = 0.5 * flux_n - 1.0
            coef[s, 4, :, rows, :] = -0.5 * flux_s - 1.0
            twelfth = 1.0 / 12.0
            e = at(aux, 0)
            slope_a = (8.0 * (at(aux, 0, 1) - at(aux, 0, -1)) - (at(aux, 0, 2) - at(aux, 0, -2))) * twelfth
            slope_b = (8.0 * (roll(e, -1, 2) - roll(e, 1, 2)) - (roll(e, -2, 2) - roll(e, 2, 2))) * twelfth
            v_e, v_w = at(state, 2, 1), at(state, 2, -1)
            turn_v = (8.0 * (v_e - v_w) - (at(state, 2, 2) - at(state, 2, -2))) * twelfth
            u_n, u_s = roll(u, -1, 2), roll(u, 1, 2)
            turn_u = (8.0 * (u_n - u_s) - (roll(u, -2, 2) - roll(u, 2, 2))) * twelfth
            spin = ((turn_v - turn_u) * inv_jac + at(stat.at[s, 1], 2)) * jac
            pair_u = at(state, 1, 1) + at(state, 1, -1)
            lap_u = (4.0 * (pair_u + (u_n + u_s)) + (roll(pair_u, -1, 2) + roll(pair_u, 1, 2)) - 20.0 * u) * (1.0 / 6.0)
            pair_v = v_e + v_w
            mid_v = 4.0 * v + pair_v
            lap_v = (4.0 * pair_v + (roll(mid_v, -1, 2) + roll(mid_v, 1, 2)) - 20.0 * v) * (1.0 / 6.0)
            u_t = spin * at(aux, 4) - slope_a + WAVE_SPEED * lap_u
            v_t = WAVE_SPEED * lap_v - spin * at(aux, 3) - slope_b
            for f, (x, x_t) in enumerate(((h, h_t), (u, u_t), (v, v_t))):
                new = x + TIME_STEP * x_t
                if now == 1:
                    new = 0.5 * (at(fresh, f) + new)
                fresh[f, :, rows, :] = new
        by_blocks(part, tile, ROWS2, PARTS2)

    def tracer_pass(s, now):
        state, fresh = tra_of[now](s), tra_of[1 - now](s)

        def part(r0):
            r0 = r0 + TOP
            rows = pl.ds(r0, ROWSB)
            g = ghost_q[s, rows, :]
            mid, east, west, north, south = (coef[s, k, :, rows, :] for k in range(5))
            scale = area[s, 1, :, rows, :]
            lane = lanes(ROWSB)
            for t in range(fields):
                q = state[t, :, rows, :]
                q_e = state[t, :, pl.ds(r0 + 1, ROWSB), :]
                q_w = state[t, :, pl.ds(r0 - 1, ROWSB), :]
                ghost = roll(g, -t, 1)
                q_n, q_s = roll(q, -1, 2), roll(q, 1, 2)
                q_s = jnp.stack([jnp.where(lane == 0, ghost, q_s[0]), q_s[1]])
                q_n = jnp.stack([q_n[0], jnp.where(lane == last_lane, ghost, q_n[1])])
                total = mid * q + (east * q_e + west * q_w) + (north * q_n + south * q_s)
                new = q + scale * total
                if now == 1:
                    new = 0.5 * (fresh[t, :, rows, :] + new)
                fresh[t, :, rows, :] = new
        by_blocks(part, tile, ROWSB, PARTSB)

    def stage(now, more):
        ends = unpack(dyn_of[now], BASE, DEPTH, of_dyn, now, ghost_d, DEPTH, True)
        unpack_corners(now, ends)

        def cells(s, carry):
            first_pass(s, now)
            second_pass(s, now)
            return carry
        lax.fori_loop(0, slots, cells, 0)

        def forward(send):
            if more is None:
                send(1 - now)
            else:
                pl.when(more)(lambda: send(1 - now))
        forward(pack_dyn)
        unpack(tra_of[now], fields, 1, of_tra, now, ghost_q, -1, False)

        def tracers_of(s, carry):
            tracer_pass(s, now)
            return carry
        lax.fori_loop(0, slots, tracers_of, 0)
        forward(pack_tra)

    def one_step(step_index, carry):
        @pl.when(step_index == STEPS // DEPTH)
        def _():
            refresh(dyn_of[0], BASE)
            refresh(tra_of[0], fields)
        stage(0, None)
        stage(1, step_index < STEPS - 1)
        return carry

    lax.fori_loop(0, STEPS, one_step, 0)


def finish(tile, dyn, tra, *outs):
    def give(src, dst):
        inner = pl.ds(TOP, tile)
        left, right = src[0, inner, :], src[1, inner, :]
        lane = lax.broadcasted_iota(jnp.int32, left.shape, 1)
        dst[:, :LANES] = jnp.where(lane < HALF, left, right)
        dst[:, LANES:] = right[:, :tile - LANES]
    for k, out in enumerate(outs[:BASE]):
        give(dyn.at[0, k], out.at[0])
    for k in range(tra.shape[1]):
        give(tra.at[0, k], outs[BASE].at[k, 0])


def coefficients(rotation, pos_a, pos_b, count, tile):
    slots = rotation.shape[0]
    line = jnp.transpose(rotation, (0, 1, 3, 4, 2)).reshape(slots, 4, 4, rotation.shape[2])
    line = jnp.pad(line, ((0, 0), (0, 0), (0, 0), (2, LANES)))
    along = lambda part, pos: lax.dynamic_slice_in_dim(part, pos * tile, 2 * LANES, axis=3)
    line = jnp.concatenate([along(line[:, 0:2], pos_b), along(line[:, 2:4], pos_a)], axis=1)
    edge = jnp.stack([pos_a == 0, pos_a == count - 1, pos_b == 0, pos_b == count - 1])
    one = jnp.array([1.0, 0.0, 0.0, 1.0], F32)[:, None]
    line = jnp.where(edge[:, None, None], line, one)
    left = jnp.concatenate([line[..., 2:LANES], line[..., 0:2]], axis=-1)
    right = jnp.concatenate([line[..., LANES + 2:LANES + 2 + TOP * TOP + DEPTH], line[..., TOP * TOP + DEPTH + 2:LANES + 2]], axis=-1)
    m = jnp.stack([left, right], axis=2)
    m = m.reshape(slots * 4, 2, 4, LANES)
    zero = jnp.zeros_like(m[:, :, 0])
    unit = jnp.ones_like(zero)
    m00, m01, m10, m11 = (m[:, :, k] for k in range(EDGES))
    stay = jnp.stack([unit, unit, m00, m00, m11, m11, zero, zero], axis=2)
    down = jnp.stack([zero, zero, zero, zero, m10, m10, zero, zero], axis=2)
    up = jnp.stack([zero, zero, m01, m01, zero, zero, zero, zero], axis=2)
    coef_e = jnp.stack([stay, down, up], axis=2)

    before, after = line[..., 1], line[..., tile + 2]
    found = []
    for k in range(EDGES):
        end_a, end_b = k // 2, k % 2
        by_a = (after if end_b else before)[:, end_a]
        by_b = (after if end_a else before)[:, 2 + end_b]
        found.append(jnp.where(edge[end_a], by_a, by_b))
    c = jnp.stack(found, axis=1).reshape(slots * 4, 4)
    zero = jnp.zeros_like(c[:, 0])
    rows = jnp.stack([jnp.stack([c[:, 0], c[:, 3]], -1), jnp.stack([zero, c[:, 2]], -1), jnp.stack([c[:, 1], zero], -1)], axis=1)
    rows = jnp.pad(rows, ((0, 0), (0, 0), (0, 6)))
    return coef_e, jnp.broadcast_to(rows[..., None], rows.shape + (LANES,))


def solution(mesh):
    cores, count = mesh.shape['panel'], mesh.shape['tx']
    slots = 6 // cores

    def body(height, wind_u, wind_v, sqrt_g, metric_aa, metric_ab, metric_bb, coriolis, topography, rotation, tracers):
        tile = height.shape[-1]
        fields = tracers.shape[0]
        coef_e, coef_c = coefficients(rotation, lax.axis_index('tx'), lax.axis_index('ty'), count, tile)
        rows = tile + DEPTH * TOP
        vmem = lambda *shape: pltpu.VMEM(shape, F32)
        blocks = (DEPTH, rows, LANES)
        state = [vmem(slots, count_f, *blocks) for count_f in (BASE, fields)]
        messages = slots * EDGES
        buffers = [vmem(DEPTH + DEPTH, messages, DEPTH, TOP, LANES), vmem(DEPTH, messages, DEPTH, TOP, LANES),
                   vmem(DEPTH, messages, TOP, LANES)]
        counters = [pltpu.SemaphoreType.DMA((count_p,)) for count_p in (DEPTH + DEPTH, DEPTH, DEPTH)]
        whole = pl.BlockSpec(memory_space=pltpu.VMEM)
        args = (height, wind_u, wind_v, sqrt_g, metric_aa, metric_ab, metric_bb, coriolis, topography, coef_e, coef_c, tracers)
        held = [jax.ShapeDtypeStruct((slots, count_f) + blocks, F32) for count_f in (BASE, fields)]
        outs = [jax.ShapeDtypeStruct(x.shape, F32) for x in (height, wind_u, wind_v, tracers)]
        call = pl.pallas_call(
            functools.partial(kernel, cores, count, tile),
            out_shape=held,
            in_specs=[whole] * len(args),
            out_specs=[whole] * len(held),
            scratch_shapes=state + [
                vmem(slots, DEPTH, BASE, *blocks), vmem(slots, DEPTH, *blocks),
                vmem(BASE + DEPTH, *blocks), vmem(slots, BASE + DEPTH, *blocks),
                vmem(DEPTH * LANES, LANES), vmem(DEPTH, LANES, LANES), vmem(slots, rows, LANES), vmem(slots, rows, LANES),
            ] + buffers * BASE + counters * DEPTH,
            compiler_params=pltpu.CompilerParams(
                collective_id=0, has_side_effects=True, vmem_limit_bytes=63 << 20),
            name='swe',
        )
        flat = pl.BlockSpec((1, tile, tile), lambda s: (s, 0, 0))
        last = pl.pallas_call(
            functools.partial(finish, tile),
            out_shape=outs,
            grid=(slots,),
            in_specs=[pl.BlockSpec((1,) + x.shape[1:], lambda s: (s,) + (0,) * len(x.shape[1:])) for x in held],
            out_specs=[flat] * BASE + [pl.BlockSpec((fields, 1, tile, tile), lambda s: (0, s, 0, 0))],
            name='finish',
        )
        return tuple(last(*call(*args)))

    state_spec = P(('member', 'panel'), 'tx', 'ty')
    static_spec = P('panel', 'tx', 'ty')
    tracer_spec = P(None, ('member', 'panel'), 'tx', 'ty')
    in_specs = (state_spec, state_spec, state_spec, static_spec, static_spec, static_spec, static_spec, static_spec, static_spec, P('panel'), tracer_spec)
    out_specs = (state_spec, state_spec, state_spec, tracer_spec)
    return jax.shard_map(body, mesh=mesh, in_specs=in_specs, out_specs=out_specs, check_vma=False)
```

```python
import functools

import jax
import jax.numpy as jnp
from jax import lax
from jax.experimental import pallas as pl
from jax.experimental.pallas import tpu as pltpu
from jax.sharding import PartitionSpec as P

STEPS = 8
TIME_STEP = 0.1
GRAVITY = 1.0
WAVE_SPEED = 1.0
LINKS = (
    '310 100 530 420',
    '010 200 511 410',
    '110 300 521 431',
    '210 000 500 401',
    '331 130 030 231',
    '320 121 221 020',
)
NEIGHBOURS = tuple(tuple(tuple(map(int, link)) for link in row.split()) for row in LINKS)
LANES = 128
HALF = 96
TOP = 8
EDGES = 4
BASE = 3
DEPTH = 2
SPLIT = 32
ROWS1, PARTS1 = 104, 1
ROWS2, PARTS2 = 48, 1
ROWSB, PARTSB = 16, 4
ROWSP = 96
F32 = jnp.float32


def pick(index, values):
    if all(value is values[0] for value in values):
        return values[0]
    total = 0
    for place, value in enumerate(values):
        total = total + same(index, place) * value
    return total


def same(x, y):
    return 1 - lax.min((x - y) * (x - y), 1)


def mix(cond, yes, no):
    return cond * yes + (1 - cond) * no


def on_edge(edge, along, count):
    if edge == 0:
        return 0, along
    if edge == 1:
        return count - 1, along
    if edge == 2:
        return along, 0
    return along, count - 1


class Plan:
    def __init__(self, core, pos_a, pos_b, cores, count):
        self.core, self.pos_a, self.pos_b = core, pos_a, pos_b
        self.cores, self.count = cores, count
        self.slots = 6 // cores
        first = lambda x: 1 - lax.div(x + count - 1, count)
        last = lambda x: lax.div(x + 1, count)
        self.at_edge = (first(pos_a), last(pos_a), first(pos_b), last(pos_b))

    def across(self, slot, edge, along, side=None):
        found = []
        for core in range(self.cores):
            other, other_edge, flipped = NEIGHBOURS[core * self.slots + slot][edge]
            place = self.count - 1 - along if flipped else along
            tile_a, tile_b = on_edge(other_edge, place, self.count)
            if side is None:
                index = (other % self.slots) * EDGES + other_edge
            else:
                end = 1 - side if flipped else side
                if other_edge < 2:
                    index = (other % self.slots) * EDGES + 2 * other_edge + end
                else:
                    index = (other % self.slots) * EDGES + 2 * end + other_edge - 2
            found.append((other // self.slots, tile_a, tile_b, index))
        return tuple(pick(self.core, [entry[k] for entry in found]) for k in range(EDGES))

    def edge(self, slot, edge):
        along = self.pos_b if edge < 2 else self.pos_a
        out = self.across(slot, edge, along)
        step = 1 if edge % 2 else -1
        inside = (
            self.core,
            self.pos_a + (step if edge < 2 else 0),
            self.pos_b + (0 if edge < 2 else step),
            slot * EDGES + (edge ^ 1),
        )
        return tuple(mix(self.at_edge[edge], o, i) for o, i in zip(out, inside))

    def corner(self, slot, end_a, end_b):
        step_a, step_b = 2 * end_a - 1, 2 * end_b - 1
        out_a, out_b = self.at_edge[end_a], self.at_edge[2 + end_b]
        by_a = self.across(slot, end_a, self.pos_b + step_b, 1 - end_b)
        by_b = self.across(slot, 2 + end_b, self.pos_a + step_a, 1 - end_a)
        inside = (self.core, self.pos_a + step_a, self.pos_b + step_b, slot * EDGES + 2 * (1 - end_a) + 1 - end_b)
        return tuple(mix(out_a, x, mix(out_b, y, z)) for x, y, z in zip(by_a, by_b, inside))

    def lone(self, end_a, end_b):
        return self.at_edge[end_a] * self.at_edge[2 + end_b]

    def here(self, found):
        return same(found[0], self.core) * same(found[1], self.pos_a) * same(found[2], self.pos_b)

    def can_stay(self, slot, edge):
        for core in range(self.cores):
            other, other_edge, flipped = NEIGHBOURS[core * self.slots + slot][edge]
            if other // self.slots == core:
                for along in range(self.count):
                    place = self.count - 1 - along if flipped else along
                    if on_edge(edge, along, self.count) == on_edge(other_edge, place, self.count):
                        return True
        return False

    def flip(self, slot, edge):
        values = [NEIGHBOURS[core * self.slots + slot][edge][2] for core in range(self.cores)]
        if not any(values):
            return None
        return self.at_edge[edge] * pick(self.core, values)


def roll(x, shift, axis):
    shift = shift % x.shape[axis]
    return x if shift == 0 else pltpu.roll(x, shift, axis)


def kernel(cores, count, tile, height, wind_u, wind_v, sqrt_g, metric_aa, metric_ab, metric_bb, coriolis,
           topography, coef_e, coef_c, tracers, dyn_a, tra_a,
           dyn_b, tra_b, stat, area, aux, coef, pack, ghost_t, ghost_d, ghost_q,
           *traffic):
    slots = 6 // cores
    fields = tracers.shape[0]
    plan = Plan(lax.axis_index('panel'), lax.axis_index('tx'), lax.axis_index('ty'), cores, count)
    edges = [[plan.edge(s, e) for e in range(EDGES)] for s in range(slots)]
    corners = [[plan.corner(s, k // 2, k % 2) for k in range(EDGES)] for s in range(slots)]
    lone = [plan.lone(k // 2, k % 2) for k in range(EDGES)]
    stays = [[plan.here(edges[s][e]) if plan.can_stay(s, e) else None for e in range(EDGES)] for s in range(slots)]
    lanes = lambda rows: lax.broadcasted_iota(jnp.int32, (rows, LANES), 1)
    lane = lanes(1)
    lane8 = lax.broadcasted_iota(jnp.int32, (8, LANES), 1)
    even8 = lax.broadcasted_iota(jnp.int32, (8, LANES), 0) % 2 == 0
    last_lane = tile - LANES - 1
    inner = pl.ds(TOP, tile)
    one = lambda k: pl.ds(k, 1)

    def where_to(found):
        return {'panel': found[0], 'tx': found[1], 'ty': found[2]}

    of_dyn, of_tra, of_end = (traffic[k::BASE] for k in range(BASE))

    def start(kind, par, index, found, stay=None):
        send, recv, spare, sent, landed = kind

        def away():
            pltpu.make_async_remote_copy(
                src_ref=send.at[par, index], dst_ref=recv.at[par, found[-1]], send_sem=sent.at[par],
                recv_sem=landed.at[par], device_id=where_to(found), device_id_type=pl.DeviceIdType.MESH).start()

        def inside():
            pltpu.make_async_copy(send.at[par, index], recv.at[par, found[-1]], landed.at[par]).start()
            pltpu.make_async_copy(send.at[par, index], spare.at[par, index], sent.at[par]).start()
        if stay is None:
            away()
        else:
            pl.when(stay == 0)(away)
            pl.when(stay == 1)(inside)

    def wait_for(kind, par):
        send, recv, _, sent, landed = kind
        pltpu.make_async_copy(recv.at[par], recv.at[par], landed.at[par]).wait()
        pltpu.make_async_copy(send.at[par], send.at[par], sent.at[par]).wait()

    of_end[1][...] = jnp.zeros_like(of_end[1])
    barrier = pltpu.get_barrier_semaphore()
    expected = 0
    for s in range(slots):
        for e in range(EDGES):
            stay = 0 if stays[s][e] is None else stays[s][e]

            def tell(s=s, e=e):
                pl.semaphore_signal(barrier, inc=1, device_id=where_to(edges[s][e]), device_id_type=pl.DeviceIdType.MESH)
            if stays[s][e] is None:
                tell()
            else:
                pl.when(stay == 0)(tell)
            expected = expected + 1 - stay
        for k in range(EDGES):
            @pl.when(lone[k] == 0)
            def _(s=s, k=k):
                pl.semaphore_signal(barrier, inc=1, device_id=where_to(corners[s][k]), device_id_type=pl.DeviceIdType.MESH)
            expected = expected + 1 - lone[k]

    def swap_pairs(x):
        return jnp.where(even8, roll(x, -1, 0), roll(x, 1, 0))

    def send_edges(kind, par, which):
        for s in range(slots):
            for e in which:
                start(kind, par, EDGES * s + e, edges[s][e], stays[s][e])

    def send_all(kind, par):
        send_edges(kind, par, range(EDGES))

    def pack_columns(src, count_f, depth, send, par):
        def step(i, carry):
            r0 = pl.multiple_of(ROWSP * i, ROWSP)
            rows = pl.ds(r0 + TOP, ROWSP)
            lane = lanes(ROWSP)
            packed = jnp.zeros((ROWSP, LANES), F32)
            for s in range(slots):
                for f in range(count_f):
                    low = TOP * s + depth * f
                    high = low + tile - LANES - depth
                    x = roll(jnp.where(lane < TOP, src(s)[f, 0, rows, :], src(s)[f, 1, rows, :]), low, 1)
                    own = (lane >= low) & (lane < low + depth) | (lane >= high) & (lane < high + depth)
                    packed = jnp.where(own, x, packed)
            packed = jnp.where(lane < SPLIT, packed, roll(packed, depth, 1))
            pack[pl.ds(r0, ROWSP), :] = packed
            return carry
        lax.fori_loop(0, tile // ROWSP, step, 0)
        turned0 = jnp.transpose(pack[:LANES])
        turned1 = jnp.transpose(pack[LANES:])
        for s in range(slots):
            for side in range(DEPTH):
                g = TOP * s + (tile - LANES) * side
                left = turned0[g:g + TOP]
                right = jnp.where(lane8 < tile - LANES, turned1[g:g + TOP], left)
                if side and depth == DEPTH:
                    left, right = swap_pairs(left), swap_pairs(right)
                index = EDGES * s + DEPTH + side
                send[par, index, 0] = left
                send[par, index, 1] = right

    def pack_rows(src, count_f, depth, send, par):
        for s in range(slots):
            for f in range(count_f):
                for d in range(depth):
                    k = one(depth * f + d)
                    send[par, EDGES * s, :, k, :] = src(s)[f, :, one(TOP + d), :]
                    send[par, EDGES * s + 1, :, k, :] = src(s)[f, :, one(tile + TOP - 1 - d), :]

    def send_corners(src, par):
        send = of_end[0]
        for s in range(slots):
            for k in range(EDGES):
                end_a, end_b = divmod(k, DEPTH)
                row = tile + TOP - 1 if end_a else TOP
                at = last_lane if end_b else 0
                for f in range(1, BASE):
                    cell = src(s)[f, end_b, one(row), one(at)]
                    send[par, EDGES * s + k, one(f - 1), :] = jnp.broadcast_to(cell, (1, LANES))
        for s in range(slots):
            for k in range(EDGES):
                found = corners[s][k]
                mine = EDGES * s + k
                start(of_end, par, mine, found[:-1] + (mix(lone[k], mine, found[-1]),), lone[k])

    def unpack(dst, count_f, depth, kind, par, ghosts, lean, turn):
        recv = kind[1]
        wait_for(kind, par)
        ends = {}
        for s in range(slots):
            for e in range(EDGES):
                index = EDGES * s + e
                left, right = recv[par, index, 0], recv[par, index, 1]
                flip = plan.flip(s, e)
                if flip is not None:
                    flipped = (jnp.zeros_like(lane8) + flip) == 1
                    mirror = lane8 ^ last_lane
                    back = jnp.take_along_axis(right, mirror, axis=1)
                    forth = jnp.take_along_axis(left, mirror, axis=1)
                    left, right = jnp.where(flipped, back, left), jnp.where(flipped, forth, right)
                if turn:
                    both = []
                    for lr, x in enumerate((left, right)):
                        stay, down, up = (coef_e[index, lr, k] for k in range(BASE))
                        both.append(stay * x + down * roll(x, DEPTH, 0) + up * roll(x, -DEPTH, 0))
                    left, right = both
                if e < DEPTH:
                    for f in range(count_f):
                        for d in range(depth):
                            k = depth * f + d
                            row = one(tile + TOP + d if e else TOP - 1 - d)
                            dst(s)[f, 0, row, :] = left[k:k + 1]
                            dst(s)[f, 1, row, :] = right[k:k + 1]
                    ends[s, e] = (left, right)
                else:
                    if e == DEPTH and depth == DEPTH:
                        left, right = swap_pairs(left), swap_pairs(right)
                    g = pl.ds(TOP * s + (tile - LANES) * (e - DEPTH), TOP)
                    ghost_t[0, g, :] = jnp.where(lane8 < HALF, left, right)
                    ghost_t[1, g, :] = right
        low = jnp.transpose(ghost_t[0])
        high = jnp.transpose(ghost_t[1])[:tile - LANES]
        low = jnp.where(lanes(LANES) < SPLIT, low, roll(low, lean, 1))
        high = jnp.where(lanes(tile - LANES) < SPLIT, high, roll(high, lean, 1))
        for s in range(slots):
            shift = -TOP * s
            ghosts[s, pl.ds(TOP, LANES), :] = roll(low, shift, 1)
            ghosts[s, pl.ds(TOP + LANES, tile - LANES), :] = roll(high, shift, 1)
        return ends

    def unpack_corners(par, ends):
        wait_for(of_end, par)
        for s in range(slots):
            rows = [jnp.zeros((1, LANES), F32)] * DEPTH
            for k in range(EDGES):
                end_a, end_b = divmod(k, DEPTH)
                x = of_end[1][par, EDGES * s + k]
                stay, down, up = (coef_c[EDGES * s + k, j] for j in range(BASE))
                x = stay * x + down * roll(x, 1, 0) + up * roll(x, -1, 0)
                alone = (jnp.zeros_like(lane) + lone[k]) == 1
                edge_row = ends[s, end_a][end_b]
                at = last_lane if end_b else 0
                for f in range(1, BASE):
                    mirrored = jnp.broadcast_to(edge_row[DEPTH * f:DEPTH * f + 1, at:at + 1], (1, LANES))
                    value = jnp.where(alone, mirrored, x[f - 1:f])
                    place = DEPTH * f + (tile - LANES + DEPTH if end_b else 1)
                    rows[end_a] = jnp.where(lane == place, value, rows[end_a])
            ghost_d[s, one(TOP - 1), :] = rows[0]
            ghost_d[s, one(tile + TOP), :] = rows[1]

    def with_columns(x, ghosts, low):
        lane = lanes(x.shape[1])
        ghosts = roll(ghosts, -DEPTH - low, 1)
        left = jnp.where(lane >= LANES - DEPTH, ghosts, x[0])
        right = jnp.where((lane == tile - LANES) | (lane == tile - LANES + 1), ghosts, x[1])
        return jnp.stack([left, right])

    def refresh(state, count_f):
        def step(f, carry):
            for s in range(slots):
                left, right = state(s)[f, 0, inner, :], state(s)[f, 1, inner, :]
                lane = lanes(tile)
                state(s)[f, 0, inner, :] = jnp.where(lane < HALF, left, right)
                state(s)[f, 1, inner, :] = jnp.where((lane < HALF) & (lane >= tile - LANES), left, right)
            return carry
        lax.fori_loop(0, count_f, step, 0)

    def take(src, dst):
        dst[0, inner, :] = src[:, :LANES]
        dst[1, inner, :] = src[:, :LANES]
        dst[1, inner, :tile - LANES] = src[:, LANES:]

    zero_rows = jnp.zeros((2 * LANES - tile, LANES), F32)
    pack[tile:2 * LANES, :] = zero_rows
    ghost_t[...] = jnp.zeros_like(ghost_t)
    ghost_d[...] = jnp.zeros_like(ghost_d)
    ghost_q[...] = jnp.zeros_like(ghost_q)
    for kind in (of_dyn, of_end):
        kind[0][...] = jnp.zeros_like(kind[0])
    group0 = lambda s: stat.at[s, 0]
    group1 = lambda s: stat.at[s, 1]
    def take_state(s, carry):
        for k, ref in enumerate((sqrt_g, metric_aa, metric_ab)):
            take(ref.at[s], stat.at[s, 0, k])
        for k, ref in enumerate((metric_bb, topography, coriolis)):
            take(ref.at[s], stat.at[s, 1, k])
        for k, ref in enumerate((height, wind_u, wind_v)):
            take(ref.at[s], dyn_a.at[s, k])
        return carry
    lax.fori_loop(0, slots, take_state, 0)
    dyn_of = {0: lambda s: dyn_a.at[s], 1: lambda s: dyn_b.at[s]}
    tra_of = {0: lambda s: tra_a.at[s], 1: lambda s: tra_b.at[s]}
    groups = (DEPTH, group0), (BASE, group1)
    for par, group in groups:
        pack_columns(group, BASE, DEPTH, of_dyn[0], par)
        pack_rows(group, BASE, DEPTH, of_dyn[0], par)
        if par == DEPTH:
            pl.semaphore_wait(barrier, expected)
        send_all(of_dyn, par)

    def pack_dyn(par):
        send_corners(dyn_of[par], par)
        pack_rows(dyn_of[par], BASE, DEPTH, of_dyn[0], par)
        send_edges(of_dyn, par, range(DEPTH))
        pack_columns(dyn_of[par], BASE, DEPTH, of_dyn[0], par)
        send_edges(of_dyn, par, range(DEPTH, EDGES))

    def pack_tra(par):
        pack_rows(tra_of[par], fields, 1, of_tra[0], par)
        send_edges(of_tra, par, range(DEPTH))
        pack_columns(tra_of[par], fields, 1, of_tra[0], par)
        send_edges(of_tra, par, range(DEPTH, EDGES))

    pack_dyn(0)
    def take_tracer(t, carry):
        for s in range(slots):
            take(tracers.at[t, s], tra_a.at[s, t])
        return carry
    lax.fori_loop(0, fields, take_tracer, 0)
    pack_tra(0)

    for par, group in groups:
        unpack(group, BASE, DEPTH, of_dyn, par, ghost_d, DEPTH, False)
        def fill_slot(s, carry):
            def fill(i, carry):
                rows = pl.ds(pl.multiple_of(ROWSP * i, ROWSP) + 8, ROWSP)
                g = ghost_d[s, rows, :]
                for f in range(3):
                    group(s)[f, :, rows, :] = with_columns(group(s)[f, :, rows, :], g, 2 * f)
                if par == DEPTH:
                    inverse = 1.0 / group(s)[0, :, rows, :]
                    area[s, 0, :, rows, :] = inverse
                    area[s, 1, :, rows, :] = (-0.5 * TIME_STEP) * inverse
                return carry
            return lax.fori_loop(0, tile // ROWSP, fill, carry)
        lax.fori_loop(0, slots, fill_slot, 0)

    def by_blocks(part, total, count_r, count_p):
        def step(i, carry):
            for k in range(count_p):
                part(pl.multiple_of(count_r * count_p * i, TOP) + count_r * k)
            return carry
        lax.fori_loop(0, total // (count_r * count_p), step, 0)

    def first_pass(s, now):
        state = dyn_of[now](s)

        def part(r0):
            rows = pl.ds(r0, ROWS1)
            g = ghost_d[s, rows, :]
            h, u, v = (with_columns(state[f, :, rows, :], g, 2 * f) for f in range(3))
            state[0, :, rows, :] = h
            state[1, :, rows, :] = u
            state[2, :, rows, :] = v
            jac, gaa, gab = (stat[s, 0, k, :, rows, :] for k in range(3))
            gbb, top = (stat[s, 1, k, :, rows, :] for k in range(2))
            contra_a = gaa * u + gab * v
            contra_b = gab * u + gbb * v
            jh = jac * h
            aux[0, :, rows, :] = GRAVITY * (h + top) + 0.5 * (u * contra_a + v * contra_b)
            aux[1, :, rows, :] = jh * contra_a
            aux[2, :, rows, :] = jh * contra_b
            aux[3, :, rows, :] = contra_a
            aux[4, :, rows, :] = contra_b
        by_blocks(part, tile + DEPTH * TOP, ROWS1, PARTS1)

    def second_pass(s, now):
        state, fresh = dyn_of[now](s), dyn_of[1 - now](s)

        def part(r0):
            r0 = r0 + TOP

            def at(ref, f, shift=0):
                return ref[f, :, pl.ds(r0 + shift, ROWS2), :]
            rows = pl.ds(r0, ROWS2)
            h, u, v = (at(state, f) for f in range(3))
            area_here = area.at[s]
            inv_jac = at(area_here, 0)
            jac = at(stat.at[s, 0], 0)
            mass_a = at(aux, 1)
            plus, minus = mass_a + h, mass_a - h
            flux_e = plus + (at(aux, 1, 1) - at(state, 0, 1))
            flux_w = (at(aux, 1, -1) + at(state, 0, -1)) + minus
            mass_b = at(aux, 2)
            plus_b, minus_b = mass_b + h, mass_b - h
            flux_n = plus_b + roll(minus_b, -1, 2)
            flux_s = roll(plus_b, 1, 2) + minus_b
            total = (flux_e - flux_w) + (flux_n - flux_s)
            h_t = (-0.5) * total * inv_jac
            coef[s, 0, :, rows, :] = 0.5 * total + 4.0
            coef[s, 1, :, rows, :] = 0.5 * flux_e - 1.0
            coef[s, 2, :, rows, :] = -0.5 * flux_w - 1.0
            coef[s, 3, :, rows, :] = 0.5 * flux_n - 1.0
            coef[s, 4, :, rows, :] = -0.5 * flux_s - 1.0
            twelfth = 1.0 / 12.0
            e = at(aux, 0)
            slope_a = (8.0 * (at(aux, 0, 1) - at(aux, 0, -1)) - (at(aux, 0, 2) - at(aux, 0, -2))) * twelfth
            slope_b = (8.0 * (roll(e, -1, 2) - roll(e, 1, 2)) - (roll(e, -2, 2) - roll(e, 2, 2))) * twelfth
            v_e, v_w = at(state, 2, 1), at(state, 2, -1)
            turn_v = (8.0 * (v_e - v_w) - (at(state, 2, 2) - at(state, 2, -2))) * twelfth
            u_n, u_s = roll(u, -1, 2), roll(u, 1, 2)
            turn_u = (8.0 * (u_n - u_s) - (roll(u, -2, 2) - roll(u, 2, 2))) * twelfth
            spin = ((turn_v - turn_u) * inv_jac + at(stat.at[s, 1], 2)) * jac
            pair_u = at(state, 1, 1) + at(state, 1, -1)
            lap_u = (4.0 * (pair_u + (u_n + u_s)) + (roll(pair_u, -1, 2) + roll(pair_u, 1, 2)) - 20.0 * u) * (1.0 / 6.0)
            pair_v = v_e + v_w
            mid_v = 4.0 * v + pair_v
            lap_v = (4.0 * pair_v + (roll(mid_v, -1, 2) + roll(mid_v, 1, 2)) - 20.0 * v) * (1.0 / 6.0)
            u_t = spin * at(aux, 4) - slope_a + WAVE_SPEED * lap_u
            v_t = WAVE_SPEED * lap_v - spin * at(aux, 3) - slope_b
            for f, (x, x_t) in enumerate(((h, h_t), (u, u_t), (v, v_t))):
                new = x + TIME_STEP * x_t
                if now == 1:
                    new = 0.5 * (at(fresh, f) + new)
                fresh[f, :, rows, :] = new
        by_blocks(part, tile, ROWS2, PARTS2)

    def tracer_pass(s, now):
        state, fresh = tra_of[now](s), tra_of[1 - now](s)

        def part(r0):
            r0 = r0 + TOP
            rows = pl.ds(r0, ROWSB)
            g = ghost_q[s, rows, :]
            mid, east, west, north, south = (coef[s, k, :, rows, :] for k in range(5))
            scale = area[s, 1, :, rows, :]
            lane = lanes(ROWSB)
            for t in range(fields):
                q = state[t, :, rows, :]
                q_e = state[t, :, pl.ds(r0 + 1, ROWSB), :]
                q_w = state[t, :, pl.ds(r0 - 1, ROWSB), :]
                ghost = roll(g, -t, 1)
                q_n, q_s = roll(q, -1, 2), roll(q, 1, 2)
                q_s = jnp.stack([jnp.where(lane == 0, ghost, q_s[0]), q_s[1]])
                q_n = jnp.stack([q_n[0], jnp.where(lane == last_lane, ghost, q_n[1])])
                total = mid * q + (east * q_e + west * q_w) + (north * q_n + south * q_s)
                new = q + scale * total
                if now == 1:
                    new = 0.5 * (fresh[t, :, rows, :] + new)
                fresh[t, :, rows, :] = new
        by_blocks(part, tile, ROWSB, PARTSB)

    def stage(now, more):
        ends = unpack(dyn_of[now], BASE, DEPTH, of_dyn, now, ghost_d, DEPTH, True)
        unpack_corners(now, ends)

        def cells(s, carry):
            first_pass(s, now)
            second_pass(s, now)
            return carry
        lax.fori_loop(0, slots, cells, 0)

        def forward(send):
            if more is None:
                send(1 - now)
            else:
                pl.when(more)(lambda: send(1 - now))
        forward(pack_dyn)
        unpack(tra_of[now], fields, 1, of_tra, now, ghost_q, -1, False)

        def tracers_of(s, carry):
            tracer_pass(s, now)
            return carry
        lax.fori_loop(0, slots, tracers_of, 0)
        forward(pack_tra)

    def one_step(step_index, carry):
        @pl.when(step_index == STEPS // DEPTH)
        def _():
            refresh(dyn_of[0], BASE)
            refresh(tra_of[0], fields)
        stage(0, None)
        stage(1, step_index < STEPS - 1)
        return carry

    lax.fori_loop(0, STEPS, one_step, 0)


def finish(tile, dyn, tra, *outs):
    def give(src, dst):
        inner = pl.ds(TOP, tile)
        left, right = src[0, inner, :], src[1, inner, :]
        lane = lax.broadcasted_iota(jnp.int32, left.shape, 1)
        dst[:, :LANES] = jnp.where(lane < HALF, left, right)
        dst[:, LANES:] = right[:, :tile - LANES]
    for k, out in enumerate(outs[:BASE]):
        give(dyn.at[0, k], out.at[0])
    for k in range(tra.shape[1]):
        give(tra.at[0, k], outs[BASE].at[k, 0])


def coefficients(rotation, pos_a, pos_b, count, tile):
    slots = rotation.shape[0]
    line = jnp.transpose(rotation, (0, 1, 3, 4, 2)).reshape(slots, 4, 4, rotation.shape[2])
    line = jnp.pad(line, ((0, 0), (0, 0), (0, 0), (2, LANES)))
    along = lambda part, pos: lax.dynamic_slice_in_dim(part, pos * tile, 2 * LANES, axis=3)
    line = jnp.concatenate([along(line[:, 0:2], pos_b), along(line[:, 2:4], pos_a)], axis=1)
    edge = jnp.stack([pos_a == 0, pos_a == count - 1, pos_b == 0, pos_b == count - 1])
    one = jnp.array([1.0, 0.0, 0.0, 1.0], F32)[:, None]
    line = jnp.where(edge[:, None, None], line, one)
    left = jnp.concatenate([line[..., 2:LANES], line[..., 0:2]], axis=-1)
    right = jnp.concatenate([line[..., LANES + 2:LANES + 2 + TOP * TOP + DEPTH], line[..., TOP * TOP + DEPTH + 2:LANES + 2]], axis=-1)
    m = jnp.stack([left, right], axis=2)
    m = m.reshape(slots * 4, 2, 4, LANES)
    zero = jnp.zeros_like(m[:, :, 0])
    unit = jnp.ones_like(zero)
    m00, m01, m10, m11 = (m[:, :, k] for k in range(EDGES))
    stay = jnp.stack([unit, unit, m00, m00, m11, m11, zero, zero], axis=2)
    down = jnp.stack([zero, zero, zero, zero, m10, m10, zero, zero], axis=2)
    up = jnp.stack([zero, zero, m01, m01, zero, zero, zero, zero], axis=2)
    coef_e = jnp.stack([stay, down, up], axis=2)

    before, after = line[..., 1], line[..., tile + 2]
    found = []
    for k in range(EDGES):
        end_a, end_b = k // 2, k % 2
        by_a = (after if end_b else before)[:, end_a]
        by_b = (after if end_a else before)[:, 2 + end_b]
        found.append(jnp.where(edge[end_a], by_a, by_b))
    c = jnp.stack(found, axis=1).reshape(slots * 4, 4)
    zero = jnp.zeros_like(c[:, 0])
    rows = jnp.stack([jnp.stack([c[:, 0], c[:, 3]], -1), jnp.stack([zero, c[:, 2]], -1), jnp.stack([c[:, 1], zero], -1)], axis=1)
    rows = jnp.pad(rows, ((0, 0), (0, 0), (0, 6)))
    return coef_e, jnp.broadcast_to(rows[..., None], rows.shape + (LANES,))


def solution(mesh):
    cores, count = mesh.shape['panel'], mesh.shape['tx']
    slots = 6 // cores

    def body(height, wind_u, wind_v, sqrt_g, metric_aa, metric_ab, metric_bb, coriolis, topography, rotation, tracers):
        tile = height.shape[-1]
        fields = tracers.shape[0]
        coef_e, coef_c = coefficients(rotation, lax.axis_index('tx'), lax.axis_index('ty'), count, tile)
        rows = tile + DEPTH * TOP
        vmem = lambda *shape: pltpu.VMEM(shape, F32)
        blocks = (DEPTH, rows, LANES)
        state = [vmem(slots, count_f, *blocks) for count_f in (BASE, fields)]
        messages = slots * EDGES
        buffers = [vmem(DEPTH + DEPTH, messages, DEPTH, TOP, LANES), vmem(DEPTH, messages, DEPTH, TOP, LANES),
                   vmem(DEPTH, messages, TOP, LANES)]
        counters = [pltpu.SemaphoreType.DMA((count_p,)) for count_p in (DEPTH + DEPTH, DEPTH, DEPTH)]
        whole = pl.BlockSpec(memory_space=pltpu.VMEM)
        args = (height, wind_u, wind_v, sqrt_g, metric_aa, metric_ab, metric_bb, coriolis, topography, coef_e, coef_c, tracers)
        held = [jax.ShapeDtypeStruct((slots, count_f) + blocks, F32) for count_f in (BASE, fields)]
        outs = [jax.ShapeDtypeStruct(x.shape, F32) for x in (height, wind_u, wind_v, tracers)]
        call = pl.pallas_call(
            functools.partial(kernel, cores, count, tile),
            out_shape=held,
            in_specs=[whole] * len(args),
            out_specs=[whole] * len(held),
            scratch_shapes=state + [
                vmem(slots, DEPTH, BASE, *blocks), vmem(slots, DEPTH, *blocks),
                vmem(BASE + DEPTH, *blocks), vmem(slots, BASE + DEPTH, *blocks),
                vmem(DEPTH * LANES, LANES), vmem(DEPTH, LANES, LANES), vmem(slots, rows, LANES), vmem(slots, rows, LANES),
            ] + buffers * BASE + counters * DEPTH,
            compiler_params=pltpu.CompilerParams(
                collective_id=0, has_side_effects=True, vmem_limit_bytes=63 << 20),
            name='swe',
        )
        flat = pl.BlockSpec((1, tile, tile), lambda s: (s, 0, 0))
        last = pl.pallas_call(
            functools.partial(finish, tile),
            out_shape=outs,
            grid=(slots,),
            in_specs=[pl.BlockSpec((1,) + x.shape[1:], lambda s: (s,) + (0,) * len(x.shape[1:])) for x in held],
            out_specs=[flat] * BASE + [pl.BlockSpec((fields, 1, tile, tile), lambda s: (0, s, 0, 0))],
            name='finish',
        )
        return tuple(last(*call(*args)))

    state_spec = P(('member', 'panel'), 'tx', 'ty')
    static_spec = P('panel', 'tx', 'ty')
    tracer_spec = P(None, ('member', 'panel'), 'tx', 'ty')
    in_specs = (state_spec, state_spec, state_spec, static_spec, static_spec, static_spec, static_spec, static_spec, static_spec, P('panel'), tracer_spec)
    out_specs = (state_spec, state_spec, state_spec, tracer_spec)
    return jax.shard_map(body, mesh=mesh, in_specs=in_specs, out_specs=out_specs, check_vma=False)
```

```python
import functools

import jax
import jax.numpy as jnp
from jax import lax
from jax.experimental import pallas as pl
from jax.experimental.pallas import tpu as pltpu
from jax.sharding import PartitionSpec as P

STEPS = 8
TIME_STEP = 0.1
GRAVITY = 1.0
WAVE_SPEED = 1.0
LINKS = (
    '310 100 530 420',
    '010 200 511 410',
    '110 300 521 431',
    '210 000 500 401',
    '331 130 030 231',
    '320 121 221 020',
)
NEIGHBOURS = tuple(tuple(tuple(map(int, link)) for link in row.split()) for row in LINKS)
LANES = 128
HALF = 96
TOP = 8
EDGES = 4
BASE = 3
DEPTH = 2
SPLIT = 32
ROWS1, PARTS1 = 104, 1
ROWS2, PARTS2 = 32, 3
ROWSB, PARTSB = 16, 4
ROWSP = 96
F32 = jnp.float32


def pick(index, values):
    if all(value is values[0] for value in values):
        return values[0]
    total = 0
    for place, value in enumerate(values):
        total = total + same(index, place) * value
    return total


def same(x, y):
    return 1 - lax.min((x - y) * (x - y), 1)


def mix(cond, yes, no):
    return cond * yes + (1 - cond) * no


def on_edge(edge, along, count):
    if edge == 0:
        return 0, along
    if edge == 1:
        return count - 1, along
    if edge == 2:
        return along, 0
    return along, count - 1


class Plan:
    def __init__(self, core, pos_a, pos_b, cores, count):
        self.core, self.pos_a, self.pos_b = core, pos_a, pos_b
        self.cores, self.count = cores, count
        self.slots = 6 // cores
        first = lambda x: 1 - lax.div(x + count - 1, count)
        last = lambda x: lax.div(x + 1, count)
        self.at_edge = (first(pos_a), last(pos_a), first(pos_b), last(pos_b))

    def across(self, slot, edge, along, side=None):
        found = []
        for core in range(self.cores):
            other, other_edge, flipped = NEIGHBOURS[core * self.slots + slot][edge]
            place = self.count - 1 - along if flipped else along
            tile_a, tile_b = on_edge(other_edge, place, self.count)
            if side is None:
                index = (other % self.slots) * EDGES + other_edge
            else:
                end = 1 - side if flipped else side
                if other_edge < 2:
                    index = (other % self.slots) * EDGES + 2 * other_edge + end
                else:
                    index = (other % self.slots) * EDGES + 2 * end + other_edge - 2
            found.append((other // self.slots, tile_a, tile_b, index))
        return tuple(pick(self.core, [entry[k] for entry in found]) for k in range(EDGES))

    def edge(self, slot, edge):
        along = self.pos_b if edge < 2 else self.pos_a
        out = self.across(slot, edge, along)
        step = 1 if edge % 2 else -1
        inside = (
            self.core,
            self.pos_a + (step if edge < 2 else 0),
            self.pos_b + (0 if edge < 2 else step),
            slot * EDGES + (edge ^ 1),
        )
        return tuple(mix(self.at_edge[edge], o, i) for o, i in zip(out, inside))

    def corner(self, slot, end_a, end_b):
        step_a, step_b = 2 * end_a - 1, 2 * end_b - 1
        out_a, out_b = self.at_edge[end_a], self.at_edge[2 + end_b]
        by_a = self.across(slot, end_a, self.pos_b + step_b, 1 - end_b)
        by_b = self.across(slot, 2 + end_b, self.pos_a + step_a, 1 - end_a)
        inside = (self.core, self.pos_a + step_a, self.pos_b + step_b, slot * EDGES + 2 * (1 - end_a) + 1 - end_b)
        return tuple(mix(out_a, x, mix(out_b, y, z)) for x, y, z in zip(by_a, by_b, inside))

    def lone(self, end_a, end_b):
        return self.at_edge[end_a] * self.at_edge[2 + end_b]

    def here(self, found):
        return same(found[0], self.core) * same(found[1], self.pos_a) * same(found[2], self.pos_b)

    def can_stay(self, slot, edge):
        for core in range(self.cores):
            other, other_edge, flipped = NEIGHBOURS[core * self.slots + slot][edge]
            if other // self.slots == core:
                for along in range(self.count):
                    place = self.count - 1 - along if flipped else along
                    if on_edge(edge, along, self.count) == on_edge(other_edge, place, self.count):
                        return True
        return False

    def flip(self, slot, edge):
        values = [NEIGHBOURS[core * self.slots + slot][edge][2] for core in range(self.cores)]
        if not any(values):
            return None
        return self.at_edge[edge] * pick(self.core, values)


def roll(x, shift, axis):
    shift = shift % x.shape[axis]
    return x if shift == 0 else pltpu.roll(x, shift, axis)


def kernel(cores, count, tile, height, wind_u, wind_v, sqrt_g, metric_aa, metric_ab, metric_bb, coriolis,
           topography, coef_e, coef_c, tracers, dyn_a, tra_a,
           dyn_b, tra_b, stat, area, aux, coef, pack, ghost_t, ghost_d, ghost_q,
           *traffic):
    slots = 6 // cores
    fields = tracers.shape[0]
    plan = Plan(lax.axis_index('panel'), lax.axis_index('tx'), lax.axis_index('ty'), cores, count)
    edges = [[plan.edge(s, e) for e in range(EDGES)] for s in range(slots)]
    corners = [[plan.corner(s, k // 2, k % 2) for k in range(EDGES)] for s in range(slots)]
    lone = [plan.lone(k // 2, k % 2) for k in range(EDGES)]
    stays = [[plan.here(edges[s][e]) if plan.can_stay(s, e) else None for e in range(EDGES)] for s in range(slots)]
    lanes = lambda rows: lax.broadcasted_iota(jnp.int32, (rows, LANES), 1)
    lane = lanes(1)
    lane8 = lax.broadcasted_iota(jnp.int32, (8, LANES), 1)
    even8 = lax.broadcasted_iota(jnp.int32, (8, LANES), 0) % 2 == 0
    last_lane = tile - LANES - 1
    inner = pl.ds(TOP, tile)
    one = lambda k: pl.ds(k, 1)

    def where_to(found):
        return {'panel': found[0], 'tx': found[1], 'ty': found[2]}

    of_dyn, of_tra, of_end = (traffic[k::BASE] for k in range(BASE))

    def start(kind, par, index, found, stay=None):
        send, recv, spare, sent, landed = kind

        def away():
            pltpu.make_async_remote_copy(
                src_ref=send.at[par, index], dst_ref=recv.at[par, found[-1]], send_sem=sent.at[par],
                recv_sem=landed.at[par], device_id=where_to(found), device_id_type=pl.DeviceIdType.MESH).start()

        def inside():
            pltpu.make_async_copy(send.at[par, index], recv.at[par, found[-1]], landed.at[par]).start()
            pltpu.make_async_copy(send.at[par, index], spare.at[par, index], sent.at[par]).start()
        if stay is None:
            away()
        else:
            pl.when(stay == 0)(away)
            pl.when(stay == 1)(inside)

    def wait_for(kind, par):
        send, recv, _, sent, landed = kind
        pltpu.make_async_copy(recv.at[par], recv.at[par], landed.at[par]).wait()
        pltpu.make_async_copy(send.at[par], send.at[par], sent.at[par]).wait()

    of_end[1][...] = jnp.zeros_like(of_end[1])
    barrier = pltpu.get_barrier_semaphore()
    expected = 0
    for s in range(slots):
        for e in range(EDGES):
            stay = 0 if stays[s][e] is None else stays[s][e]

            def tell(s=s, e=e):
                pl.semaphore_signal(barrier, inc=1, device_id=where_to(edges[s][e]), device_id_type=pl.DeviceIdType.MESH)
            if stays[s][e] is None:
                tell()
            else:
                pl.when(stay == 0)(tell)
            expected = expected + 1 - stay
        for k in range(EDGES):
            @pl.when(lone[k] == 0)
            def _(s=s, k=k):
                pl.semaphore_signal(barrier, inc=1, device_id=where_to(corners[s][k]), device_id_type=pl.DeviceIdType.MESH)
            expected = expected + 1 - lone[k]

    def swap_pairs(x):
        return jnp.where(even8, roll(x, -1, 0), roll(x, 1, 0))

    def send_all(kind, par):
        for s in range(slots):
            for e in range(EDGES):
                start(kind, par, EDGES * s + e, edges[s][e], stays[s][e])

    def pack_columns(src, count_f, depth, send, par):
        def step(i, carry):
            r0 = pl.multiple_of(ROWSP * i, ROWSP)
            rows = pl.ds(r0 + TOP, ROWSP)
            lane = lanes(ROWSP)
            packed = jnp.zeros((ROWSP, LANES), F32)
            for s in range(slots):
                for f in range(count_f):
                    low = TOP * s + depth * f
                    high = low + tile - LANES - depth
                    x = roll(jnp.where(lane < TOP, src(s)[f, 0, rows, :], src(s)[f, 1, rows, :]), low, 1)
                    own = (lane >= low) & (lane < low + depth) | (lane >= high) & (lane < high + depth)
                    packed = jnp.where(own, x, packed)
            packed = jnp.where(lane < SPLIT, packed, roll(packed, depth, 1))
            pack[pl.ds(r0, ROWSP), :] = packed
            return carry
        lax.fori_loop(0, tile // ROWSP, step, 0)
        turned0 = jnp.transpose(pack[:LANES])
        turned1 = jnp.transpose(pack[LANES:])
        for s in range(slots):
            for side in range(DEPTH):
                g = TOP * s + (tile - LANES) * side
                left = turned0[g:g + TOP]
                right = jnp.where(lane8 < tile - LANES, turned1[g:g + TOP], left)
                if side and depth == DEPTH:
                    left, right = swap_pairs(left), swap_pairs(right)
                index = EDGES * s + DEPTH + side
                send[par, index, 0] = left
                send[par, index, 1] = right

    def pack_rows(src, count_f, depth, send, par):
        for s in range(slots):
            for f in range(count_f):
                for d in range(depth):
                    k = one(depth * f + d)
                    send[par, EDGES * s, :, k, :] = src(s)[f, :, one(TOP + d), :]
                    send[par, EDGES * s + 1, :, k, :] = src(s)[f, :, one(tile + TOP - 1 - d), :]

    def send_corners(src, par):
        send = of_end[0]
        for s in range(slots):
            for k in range(EDGES):
                end_a, end_b = divmod(k, DEPTH)
                row = tile + TOP - 1 if end_a else TOP
                at = last_lane if end_b else 0
                for f in range(1, BASE):
                    cell = src(s)[f, end_b, one(row), one(at)]
                    send[par, EDGES * s + k, one(f - 1), :] = jnp.broadcast_to(cell, (1, LANES))
        for s in range(slots):
            for k in range(EDGES):
                found = corners[s][k]
                mine = EDGES * s + k
                start(of_end, par, mine, found[:-1] + (mix(lone[k], mine, found[-1]),), lone[k])

    def unpack(dst, count_f, depth, kind, par, ghosts, lean, turn):
        recv = kind[1]
        wait_for(kind, par)
        ends = {}
        for s in range(slots):
            for e in range(EDGES):
                index = EDGES * s + e
                left, right = recv[par, index, 0], recv[par, index, 1]
                flip = plan.flip(s, e)
                if flip is not None:
                    flipped = (jnp.zeros_like(lane8) + flip) == 1
                    mirror = lane8 ^ last_lane
                    back = jnp.take_along_axis(right, mirror, axis=1)
                    forth = jnp.take_along_axis(left, mirror, axis=1)
                    left, right = jnp.where(flipped, back, left), jnp.where(flipped, forth, right)
                if turn:
                    both = []
                    for lr, x in enumerate((left, right)):
                        stay, down, up = (coef_e[index, lr, k] for k in range(BASE))
                        both.append(stay * x + down * roll(x, DEPTH, 0) + up * roll(x, -DEPTH, 0))
                    left, right = both
                if e < DEPTH:
                    for f in range(count_f):
                        for d in range(depth):
                            k = depth * f + d
                            row = one(tile + TOP + d if e else TOP - 1 - d)
                            dst(s)[f, 0, row, :] = left[k:k + 1]
                            dst(s)[f, 1, row, :] = right[k:k + 1]
                    ends[s, e] = (left, right)
                else:
                    if e == DEPTH and depth == DEPTH:
                        left, right = swap_pairs(left), swap_pairs(right)
                    g = pl.ds(TOP * s + (tile - LANES) * (e - DEPTH), TOP)
                    ghost_t[0, g, :] = jnp.where(lane8 < HALF, left, right)
                    ghost_t[1, g, :] = right
        low = jnp.transpose(ghost_t[0])
        high = jnp.transpose(ghost_t[1])[:tile - LANES]
        low = jnp.where(lanes(LANES) < SPLIT, low, roll(low, lean, 1))
        high = jnp.where(lanes(tile - LANES) < SPLIT, high, roll(high, lean, 1))
        for s in range(slots):
            shift = -TOP * s
            ghosts[s, pl.ds(TOP, LANES), :] = roll(low, shift, 1)
            ghosts[s, pl.ds(TOP + LANES, tile - LANES), :] = roll(high, shift, 1)
        return ends

    def unpack_corners(par, ends):
        wait_for(of_end, par)
        for s in range(slots):
            rows = [jnp.zeros((1, LANES), F32)] * DEPTH
            for k in range(EDGES):
                end_a, end_b = divmod(k, DEPTH)
                x = of_end[1][par, EDGES * s + k]
                stay, down, up = (coef_c[EDGES * s + k, j] for j in range(BASE))
                x = stay * x + down * roll(x, 1, 0) + up * roll(x, -1, 0)
                alone = (jnp.zeros_like(lane) + lone[k]) == 1
                edge_row = ends[s, end_a][end_b]
                at = last_lane if end_b else 0
                for f in range(1, BASE):
                    mirrored = jnp.broadcast_to(edge_row[DEPTH * f:DEPTH * f + 1, at:at + 1], (1, LANES))
                    value = jnp.where(alone, mirrored, x[f - 1:f])
                    place = DEPTH * f + (tile - LANES + DEPTH if end_b else 1)
                    rows[end_a] = jnp.where(lane == place, value, rows[end_a])
            ghost_d[s, one(TOP - 1), :] = rows[0]
            ghost_d[s, one(tile + TOP), :] = rows[1]

    def with_columns(x, ghosts, low):
        lane = lanes(x.shape[1])
        ghosts = roll(ghosts, -DEPTH - low, 1)
        left = jnp.where(lane >= LANES - DEPTH, ghosts, x[0])
        right = jnp.where((lane == tile - LANES) | (lane == tile - LANES + 1), ghosts, x[1])
        return jnp.stack([left, right])

    def refresh(state, count_f):
        def step(f, carry):
            for s in range(slots):
                left, right = state(s)[f, 0, inner, :], state(s)[f, 1, inner, :]
                lane = lanes(tile)
                state(s)[f, 0, inner, :] = jnp.where(lane < HALF, left, right)
                state(s)[f, 1, inner, :] = jnp.where((lane < HALF) & (lane >= tile - LANES), left, right)
            return carry
        lax.fori_loop(0, count_f, step, 0)

    def take(src, dst):
        dst[0, inner, :] = src[:, :LANES]
        dst[1, inner, :] = src[:, :LANES]
        dst[1, inner, :tile - LANES] = src[:, LANES:]

    zero_rows = jnp.zeros((2 * LANES - tile, LANES), F32)
    pack[tile:2 * LANES, :] = zero_rows
    ghost_t[...] = jnp.zeros_like(ghost_t)
    ghost_d[...] = jnp.zeros_like(ghost_d)
    ghost_q[...] = jnp.zeros_like(ghost_q)
    for kind in (of_dyn, of_end):
        kind[0][...] = jnp.zeros_like(kind[0])
    group0 = lambda s: stat.at[s, 0]
    group1 = lambda s: stat.at[s, 1]
    def take_state(s, carry):
        for k, ref in enumerate((sqrt_g, metric_aa, metric_ab)):
            take(ref.at[s], stat.at[s, 0, k])
        for k, ref in enumerate((metric_bb, topography, coriolis)):
            take(ref.at[s], stat.at[s, 1, k])
        for k, ref in enumerate((height, wind_u, wind_v)):
            take(ref.at[s], dyn_a.at[s, k])
        return carry
    lax.fori_loop(0, slots, take_state, 0)
    dyn_of = {0: lambda s: dyn_a.at[s], 1: lambda s: dyn_b.at[s]}
    tra_of = {0: lambda s: tra_a.at[s], 1: lambda s: tra_b.at[s]}
    groups = (DEPTH, group0), (BASE, group1)
    for par, group in groups:
        pack_columns(group, BASE, DEPTH, of_dyn[0], par)
        pack_rows(group, BASE, DEPTH, of_dyn[0], par)
        if par == DEPTH:
            pl.semaphore_wait(barrier, expected)
        send_all(of_dyn, par)

    def pack_dyn(par):
        pack_columns(dyn_of[par], BASE, DEPTH, of_dyn[0], par)
        pack_rows(dyn_of[par], BASE, DEPTH, of_dyn[0], par)
        send_all(of_dyn, par)
        send_corners(dyn_of[par], par)

    def pack_tra(par):
        pack_columns(tra_of[par], fields, 1, of_tra[0], par)
        pack_rows(tra_of[par], fields, 1, of_tra[0], par)
        send_all(of_tra, par)

    pack_dyn(0)
    def take_tracer(t, carry):
        for s in range(slots):
            take(tracers.at[t, s], tra_a.at[s, t])
        return carry
    lax.fori_loop(0, fields, take_tracer, 0)
    pack_tra(0)

    for par, group in groups:
        unpack(group, BASE, DEPTH, of_dyn, par, ghost_d, DEPTH, False)
        def fill_slot(s, carry):
            def fill(i, carry):
                rows = pl.ds(pl.multiple_of(ROWSP * i, ROWSP) + 8, ROWSP)
                g = ghost_d[s, rows, :]
                for f in range(3):
                    group(s)[f, :, rows, :] = with_columns(group(s)[f, :, rows, :], g, 2 * f)
                if par == DEPTH:
                    inverse = 1.0 / group(s)[0, :, rows, :]
                    area[s, 0, :, rows, :] = inverse
                    area[s, 1, :, rows, :] = (-0.5 * TIME_STEP) * inverse
                return carry
            return lax.fori_loop(0, tile // ROWSP, fill, carry)
        lax.fori_loop(0, slots, fill_slot, 0)

    def by_blocks(part, total, count_r, count_p):
        def step(i, carry):
            for k in range(count_p):
                part(pl.multiple_of(count_r * count_p * i, TOP) + count_r * k)
            return carry
        lax.fori_loop(0, total // (count_r * count_p), step, 0)

    def first_pass(s, now):
        state = dyn_of[now](s)

        def part(r0):
            rows = pl.ds(r0, ROWS1)
            g = ghost_d[s, rows, :]
            h, u, v = (with_columns(state[f, :, rows, :], g, 2 * f) for f in range(3))
            state[0, :, rows, :] = h
            state[1, :, rows, :] = u
            state[2, :, rows, :] = v
            jac, gaa, gab = (stat[s, 0, k, :, rows, :] for k in range(3))
            gbb, top = (stat[s, 1, k, :, rows, :] for k in range(2))
            contra_a = gaa * u + gab * v
            contra_b = gab * u + gbb * v
            jh = jac * h
            aux[0, :, rows, :] = GRAVITY * (h + top) + 0.5 * (u * contra_a + v * contra_b)
            aux[1, :, rows, :] = jh * contra_a
            aux[2, :, rows, :] = jh * contra_b
            aux[3, :, rows, :] = contra_a
            aux[4, :, rows, :] = contra_b
        by_blocks(part, tile + DEPTH * TOP, ROWS1, PARTS1)

    def second_pass(s, now):
        state, fresh = dyn_of[now](s), dyn_of[1 - now](s)

        def part(r0):
            r0 = r0 + TOP

            def at(ref, f, shift=0):
                return ref[f, :, pl.ds(r0 + shift, ROWS2), :]
            rows = pl.ds(r0, ROWS2)
            h, u, v = (at(state, f) for f in range(3))
            area_here = area.at[s]
            inv_jac = at(area_here, 0)
            jac = at(stat.at[s, 0], 0)
            mass_a = at(aux, 1)
            plus, minus = mass_a + h, mass_a - h
            flux_e = plus + (at(aux, 1, 1) - at(state, 0, 1))
            flux_w = (at(aux, 1, -1) + at(state, 0, -1)) + minus
            mass_b = at(aux, 2)
            plus_b, minus_b = mass_b + h, mass_b - h
            flux_n = plus_b + roll(minus_b, -1, 2)
            flux_s = roll(plus_b, 1, 2) + minus_b
            total = (flux_e - flux_w) + (flux_n - flux_s)
            h_t = (-0.5) * total * inv_jac
            coef[s, 0, :, rows, :] = 0.5 * total + 4.0
            coef[s, 1, :, rows, :] = 0.5 * flux_e - 1.0
            coef[s, 2, :, rows, :] = -0.5 * flux_w - 1.0
            coef[s, 3, :, rows, :] = 0.5 * flux_n - 1.0
            coef[s, 4, :, rows, :] = -0.5 * flux_s - 1.0
            twelfth = 1.0 / 12.0
            e = at(aux, 0)
            slope_a = (8.0 * (at(aux, 0, 1) - at(aux, 0, -1)) - (at(aux, 0, 2) - at(aux, 0, -2))) * twelfth
            slope_b = (8.0 * (roll(e, -1, 2) - roll(e, 1, 2)) - (roll(e, -2, 2) - roll(e, 2, 2))) * twelfth
            v_e, v_w = at(state, 2, 1), at(state, 2, -1)
            turn_v = (8.0 * (v_e - v_w) - (at(state, 2, 2) - at(state, 2, -2))) * twelfth
            u_n, u_s = roll(u, -1, 2), roll(u, 1, 2)
            turn_u = (8.0 * (u_n - u_s) - (roll(u, -2, 2) - roll(u, 2, 2))) * twelfth
            spin = ((turn_v - turn_u) * inv_jac + at(stat.at[s, 1], 2)) * jac
            pair_u = at(state, 1, 1) + at(state, 1, -1)
            lap_u = (4.0 * (pair_u + (u_n + u_s)) + (roll(pair_u, -1, 2) + roll(pair_u, 1, 2)) - 20.0 * u) * (1.0 / 6.0)
            pair_v = v_e + v_w
            mid_v = 4.0 * v + pair_v
            lap_v = (4.0 * pair_v + (roll(mid_v, -1, 2) + roll(mid_v, 1, 2)) - 20.0 * v) * (1.0 / 6.0)
            u_t = spin * at(aux, 4) - slope_a + WAVE_SPEED * lap_u
            v_t = WAVE_SPEED * lap_v - spin * at(aux, 3) - slope_b
            for f, (x, x_t) in enumerate(((h, h_t), (u, u_t), (v, v_t))):
                new = x + TIME_STEP * x_t
                if now == 1:
                    new = 0.5 * (at(fresh, f) + new)
                fresh[f, :, rows, :] = new
        by_blocks(part, tile, ROWS2, PARTS2)

    def tracer_pass(s, now):
        state, fresh = tra_of[now](s), tra_of[1 - now](s)

        def part(r0):
            r0 = r0 + TOP
            rows = pl.ds(r0, ROWSB)
            g = ghost_q[s, rows, :]
            mid, east, west, north, south = (coef[s, k, :, rows, :] for k in range(5))
            scale = area[s, 1, :, rows, :]
            lane = lanes(ROWSB)
            for t in range(fields):
                q = state[t, :, rows, :]
                q_e = state[t, :, pl.ds(r0 + 1, ROWSB), :]
                q_w = state[t, :, pl.ds(r0 - 1, ROWSB), :]
                ghost = roll(g, -t, 1)
                q_n, q_s = roll(q, -1, 2), roll(q, 1, 2)
                q_s = jnp.stack([jnp.where(lane == 0, ghost, q_s[0]), q_s[1]])
                q_n = jnp.stack([q_n[0], jnp.where(lane == last_lane, ghost, q_n[1])])
                total = mid * q + (east * q_e + west * q_w) + (north * q_n + south * q_s)
                new = q + scale * total
                if now == 1:
                    new = 0.5 * (fresh[t, :, rows, :] + new)
                fresh[t, :, rows, :] = new
        by_blocks(part, tile, ROWSB, PARTSB)

    def stage(now, more):
        ends = unpack(dyn_of[now], BASE, DEPTH, of_dyn, now, ghost_d, DEPTH, True)
        unpack_corners(now, ends)

        def cells(s, carry):
            first_pass(s, now)
            second_pass(s, now)
            return carry
        lax.fori_loop(0, slots, cells, 0)

        def forward(send):
            if more is None:
                send(1 - now)
            else:
                pl.when(more)(lambda: send(1 - now))
        forward(pack_dyn)
        unpack(tra_of[now], fields, 1, of_tra, now, ghost_q, -1, False)

        def tracers_of(s, carry):
            tracer_pass(s, now)
            return carry
        lax.fori_loop(0, slots, tracers_of, 0)
        forward(pack_tra)

    def one_step(step_index, carry):
        @pl.when(step_index == STEPS // DEPTH)
        def _():
            refresh(dyn_of[0], BASE)
            refresh(tra_of[0], fields)
        stage(0, None)
        stage(1, step_index < STEPS - 1)
        return carry

    lax.fori_loop(0, STEPS, one_step, 0)


def finish(tile, dyn, tra, *outs):
    def give(src, dst):
        inner = pl.ds(TOP, tile)
        left, right = src[0, inner, :], src[1, inner, :]
        lane = lax.broadcasted_iota(jnp.int32, left.shape, 1)
        dst[:, :LANES] = jnp.where(lane < HALF, left, right)
        dst[:, LANES:] = right[:, :tile - LANES]
    for k, out in enumerate(outs[:BASE]):
        give(dyn.at[0, k], out.at[0])
    for k in range(tra.shape[1]):
        give(tra.at[0, k], outs[BASE].at[k, 0])


def coefficients(rotation, pos_a, pos_b, count, tile):
    slots = rotation.shape[0]
    line = jnp.transpose(rotation, (0, 1, 3, 4, 2)).reshape(slots, 4, 4, rotation.shape[2])
    line = jnp.pad(line, ((0, 0), (0, 0), (0, 0), (2, LANES)))
    along = lambda part, pos: lax.dynamic_slice_in_dim(part, pos * tile, 2 * LANES, axis=3)
    line = jnp.concatenate([along(line[:, 0:2], pos_b), along(line[:, 2:4], pos_a)], axis=1)
    edge = jnp.stack([pos_a == 0, pos_a == count - 1, pos_b == 0, pos_b == count - 1])
    one = jnp.array([1.0, 0.0, 0.0, 1.0], F32)[:, None]
    line = jnp.where(edge[:, None, None], line, one)
    left = jnp.concatenate([line[..., 2:LANES], line[..., 0:2]], axis=-1)
    right = jnp.concatenate([line[..., LANES + 2:LANES + 2 + TOP * TOP + DEPTH], line[..., TOP * TOP + DEPTH + 2:LANES + 2]], axis=-1)
    m = jnp.stack([left, right], axis=2)
    m = m.reshape(slots * 4, 2, 4, LANES)
    zero = jnp.zeros_like(m[:, :, 0])
    unit = jnp.ones_like(zero)
    m00, m01, m10, m11 = (m[:, :, k] for k in range(EDGES))
    stay = jnp.stack([unit, unit, m00, m00, m11, m11, zero, zero], axis=2)
    down = jnp.stack([zero, zero, zero, zero, m10, m10, zero, zero], axis=2)
    up = jnp.stack([zero, zero, m01, m01, zero, zero, zero, zero], axis=2)
    coef_e = jnp.stack([stay, down, up], axis=2)

    before, after = line[..., 1], line[..., tile + 2]
    found = []
    for k in range(EDGES):
        end_a, end_b = k // 2, k % 2
        by_a = (after if end_b else before)[:, end_a]
        by_b = (after if end_a else before)[:, 2 + end_b]
        found.append(jnp.where(edge[end_a], by_a, by_b))
    c = jnp.stack(found, axis=1).reshape(slots * 4, 4)
    zero = jnp.zeros_like(c[:, 0])
    rows = jnp.stack([jnp.stack([c[:, 0], c[:, 3]], -1), jnp.stack([zero, c[:, 2]], -1), jnp.stack([c[:, 1], zero], -1)], axis=1)
    rows = jnp.pad(rows, ((0, 0), (0, 0), (0, 6)))
    return coef_e, jnp.broadcast_to(rows[..., None], rows.shape + (LANES,))


def solution(mesh):
    cores, count = mesh.shape['panel'], mesh.shape['tx']
    slots = 6 // cores

    def body(height, wind_u, wind_v, sqrt_g, metric_aa, metric_ab, metric_bb, coriolis, topography, rotation, tracers):
        tile = height.shape[-1]
        fields = tracers.shape[0]
        coef_e, coef_c = coefficients(rotation, lax.axis_index('tx'), lax.axis_index('ty'), count, tile)
        rows = tile + DEPTH * TOP
        vmem = lambda *shape: pltpu.VMEM(shape, F32)
        blocks = (DEPTH, rows, LANES)
        state = [vmem(slots, count_f, *blocks) for count_f in (BASE, fields)]
        messages = slots * EDGES
        buffers = [vmem(DEPTH + DEPTH, messages, DEPTH, TOP, LANES), vmem(DEPTH, messages, DEPTH, TOP, LANES),
                   vmem(DEPTH, messages, TOP, LANES)]
        counters = [pltpu.SemaphoreType.DMA((count_p,)) for count_p in (DEPTH + DEPTH, DEPTH, DEPTH)]
        whole = pl.BlockSpec(memory_space=pltpu.VMEM)
        args = (height, wind_u, wind_v, sqrt_g, metric_aa, metric_ab, metric_bb, coriolis, topography, coef_e, coef_c, tracers)
        held = [jax.ShapeDtypeStruct((slots, count_f) + blocks, F32) for count_f in (BASE, fields)]
        outs = [jax.ShapeDtypeStruct(x.shape, F32) for x in (height, wind_u, wind_v, tracers)]
        call = pl.pallas_call(
            functools.partial(kernel, cores, count, tile),
            out_shape=held,
            in_specs=[whole] * len(args),
            out_specs=[whole] * len(held),
            scratch_shapes=state + [
                vmem(slots, DEPTH, BASE, *blocks), vmem(slots, DEPTH, *blocks),
                vmem(BASE + DEPTH, *blocks), vmem(slots, BASE + DEPTH, *blocks),
                vmem(DEPTH * LANES, LANES), vmem(DEPTH, LANES, LANES), vmem(slots, rows, LANES), vmem(slots, rows, LANES),
            ] + buffers * BASE + counters * DEPTH,
            compiler_params=pltpu.CompilerParams(
                collective_id=0, has_side_effects=True, vmem_limit_bytes=63 << 20),
            name='swe',
        )
        flat = pl.BlockSpec((1, tile, tile), lambda s: (s, 0, 0))
        last = pl.pallas_call(
            functools.partial(finish, tile),
            out_shape=outs,
            grid=(slots,),
            in_specs=[pl.BlockSpec((1,) + x.shape[1:], lambda s: (s,) + (0,) * len(x.shape[1:])) for x in held],
            out_specs=[flat] * BASE + [pl.BlockSpec((fields, 1, tile, tile), lambda s: (0, s, 0, 0))],
            name='finish',
        )
        return tuple(last(*call(*args)))

    state_spec = P(('member', 'panel'), 'tx', 'ty')
    static_spec = P('panel', 'tx', 'ty')
    tracer_spec = P(None, ('member', 'panel'), 'tx', 'ty')
    in_specs = (state_spec, state_spec, state_spec, static_spec, static_spec, static_spec, static_spec, static_spec, static_spec, P('panel'), tracer_spec)
    out_specs = (state_spec, state_spec, state_spec, tracer_spec)
    return jax.shard_map(body, mesh=mesh, in_specs=in_specs, out_specs=out_specs, check_vma=False)
```
